32 devices in a mesh: tm: 4 (over z), sx: 4 (over y, x), sy: 2 (over core).
Axes of the slice: x: 2, y: 2, z: 4, core: 2. Of those that a mesh axis runs over, the one named last changes fastest.
Arguments:
- thickness_guess: float32 [4, 1024, 256], P('tm', 'sx', 'sy'), may hold values from 0.5 to 1.5
- thickness_start: float32 [1024, 256], P('sx', 'sy'), may hold values from 0.5 to 1.5
- bed: float32 [1024, 256], P('sx', 'sy'), may hold values from -1.8 to 1.8
- rate_factor: float32 [1024, 256], P('sx', 'sy'), may hold values from 0.05 to 0.5
- mass_balance: float32 [4, 1024, 256], P('tm', 'sx', 'sy'), may hold values from -1.2 to 1.2
- cell_flags: int32 [1024, 256], P('sx', 'sy'), may hold values from 0 to 2, as said below
Outputs:
- thickness: float32 [4, 1024, 256], P('tm', 'sx', 'sy')
The draws below stay inside these ranges and needn't reach their ends.
Inputs may be any that keep to these rules, and one draw needn't show every extreme that they name: `cell_flags`: 0 marks ice-free cells outside the glacier, 1 ice on bedrock, 2 ice on soft sediment.
All inputs are finite; a program needn't handle non-finite values.
Results may differ from the reference program's by a relative error of at most 0.00015.
Values sent between devices are 32-bit elements; how exact they have to be, the bound alone decides.
No kernel may reach another device: no remote copies, remote signals or barrier semaphores. Data moves between devices by JAX's collectives and lax.ppermute only.
A program may use at most 64 MiB of HBM per device.

```python
import math
import jax
import jax.numpy as jnp
from jax import lax

NEWTON = 2
SWEEPS = 8
LEVELS = 4
NX = 1024
NY = 256


def ellipse_union(key, members, narrow, broad):
    keys = jax.random.split(key, 4)
    row_grid = lax.broadcasted_iota(jnp.int32, (NX, NY), 0)
    col_grid = lax.broadcasted_iota(jnp.int32, (NX, NY), 1)
    centre_row = jax.random.randint(keys[0], (members,), 0, NX)
    centre_col = jax.random.randint(keys[1], (members,), 0, NY)
    radius_row = jax.random.randint(keys[2], (members,), max(NX // narrow, 1), max(NX // broad, 2))
    radius_col = jax.random.randint(keys[3], (members,), max(NY // narrow, 1), max(NY // broad, 2))
    covered = jnp.zeros((NX, NY), jnp.int32)
    for member in range(members):
        reach_row = row_grid - centre_row[member]
        reach_col = col_grid - centre_col[member]
        measure = reach_row * reach_row * 256 // (radius_row[member] * radius_row[member]) + reach_col * reach_col * 256 // (radius_col[member] * radius_col[member])
        covered = jnp.maximum(covered, (measure <= 256).astype(jnp.int32))
    return covered


def draw_cell_flags(key, part):
    base = jax.random.fold_in(key, 11)
    glacier = ellipse_union(jax.random.fold_in(base, 1), 12, 8, 4)
    sediment = ellipse_union(jax.random.fold_in(base, 2), 8, 16, 8)
    return (glacier * (1 + sediment)).astype(jnp.int32)


def block_scale(rng, shape, cuts, least, largest):
    def one(dim, shards_of):
        draws = jax.random.uniform(jax.random.fold_in(jax.random.fold_in(rng, 6), dim), (shards_of,), jnp.float32, least / len(cuts), largest / len(cuts))
        return jnp.repeat(jnp.exp(draws), shape[dim] // shards_of).reshape((-1,) + (1,) * (len(shape) - dim - 1))

    loudness = one(*cuts[0])
    for cut in cuts[1:]:
        loudness = loudness * one(*cut)
    return loudness


def gaussian(key, extent, width, limit, cuts=(), dtype=jnp.bfloat16):
    array = jax.random.normal(key, extent, jnp.float32) * width
    if len(cuts) > 0:
        array = block_scale(key, extent, cuts, -0.22, 0.18) * array
    return jnp.clip(array, min=-limit, max=limit).astype(dtype)


def setup_inputs(seed: int = 0) -> dict:
    splits = jax.random.split(jax.random.key(seed), 7)
    return {
        "thickness_guess": jnp.clip(0.5 + 1.0 * jax.random.uniform(splits[0], (LEVELS, NX, NY), jnp.float32) ** block_scale(splits[0], (LEVELS, NX, NY), ((0, 4), (1, 4), (2, 2)), -0.2, 0.2), 0.5, 1.5),
        "thickness_start": jnp.clip(0.5 + 1.0 * jax.random.uniform(splits[1], (NX, NY), jnp.float32) ** block_scale(splits[1], (NX, NY), ((0, 4), (1, 2)), -0.2, 0.2), 0.5, 1.5),
        "bed": gaussian(splits[2], (NX, NY), 0.3, 1.8, ((0, 4), (1, 2)), jnp.float32),
        "rate_factor": jnp.clip(jnp.exp(math.log(0.5) - 2.3025851 * jax.random.uniform(splits[3], (NX, NY), jnp.float32) ** block_scale(splits[3], (NX, NY), ((0, 4), (1, 2)), -0.2, 0.2)), 0.05, 0.5),
        "mass_balance": gaussian(splits[4], (LEVELS, NX, NY), 0.2, 1.2, ((0, 4), (1, 4), (2, 2)), jnp.float32),
        "cell_flags": draw_cell_flags(jax.random.fold_in(splits[6], 71), 0),
    }


circulant_weight = 0.25
time_step = 1.0


def cell_diffusivity(thickness, rate_factor, cell_flags):
    inside = (cell_flags != 0).astype(jnp.float32)
    boost = 1.0 + (cell_flags == 2).astype(jnp.float32)
    return inside * boost * rate_factor * thickness * thickness * jnp.abs(thickness)


def face_weights(padded):
    centre = padded[1:-1, 1:-1]
    return (0.5 * (centre + padded[2:, 1:-1]), 0.5 * (centre + padded[:-2, 1:-1]),
            0.5 * (centre + padded[1:-1, 2:]), 0.5 * (centre + padded[1:-1, :-2]))


def neighbour_sum(weights, padded):
    return (weights[0] * padded[2:, 1:-1] + weights[1] * padded[:-2, 1:-1]
            + weights[2] * padded[1:-1, 2:] + weights[3] * padded[1:-1, :-2])


def reference(thickness_guess, thickness_start, bed, rate_factor, mass_balance, cell_flags):
    levels = thickness_guess.shape[0]
    inside = (cell_flags != 0).astype(jnp.float32)
    ratio_root = circulant_weight ** (1.0 / levels)
    level_range = jnp.arange(levels).astype(jnp.float32)
    weight_up = ratio_root ** level_range
    mode_angle = (2.0 * math.pi / levels) * level_range
    shift_real = (1.0 - ratio_root * jnp.cos(mode_angle)) / time_step
    shift_imag = ratio_root * jnp.sin(mode_angle) / time_step
    thickness = thickness_guess
    for newton_step in range(NEWTON):
        prior_level = jnp.concatenate([thickness_start[None], thickness[:-1]], 0)

        def residual_of(operands):
            level_thickness, level_prior, level_balance = operands
            diffuse = cell_diffusivity(level_thickness, rate_factor, cell_flags)
            weights = face_weights(jnp.pad(diffuse, 1))
            face_total = weights[0] + weights[1] + weights[2] + weights[3]
            surface = level_thickness + bed
            change = ((level_thickness - level_prior) / time_step + face_total * surface
                      - neighbour_sum(weights, jnp.pad(surface, 1)) - level_balance)
            return inside * change, diffuse

        residual, diffuse = lax.map(residual_of, (thickness, prior_level, mass_balance))
        mean_diff = jnp.sum(diffuse, axis=0) / levels
        weights = face_weights(jnp.pad(mean_diff, 1))
        face_total = weights[0] + weights[1] + weights[2] + weights[3]
        spectrum = jnp.fft.fft(residual * weight_up[:, None, None], axis=0)
        spectrum_real = jnp.real(spectrum)
        spectrum_imag = jnp.imag(spectrum)

        def solve_mode(operands):
            source_real, source_imag, one_real, one_imag = operands
            denom_real = one_real + face_total
            denom_norm = denom_real * denom_real + one_imag * one_imag
            inverse_real = inside * denom_real / denom_norm
            inverse_imag = -inside * one_imag / denom_norm
            value_real = source_real * inverse_real - source_imag * inverse_imag
            value_imag = source_real * inverse_imag + source_imag * inverse_real
            for sweep_index in range(SWEEPS - 1):
                numer_real = source_real + neighbour_sum(weights, jnp.pad(value_real, 1))
                numer_imag = source_imag + neighbour_sum(weights, jnp.pad(value_imag, 1))
                value_real = numer_real * inverse_real - numer_imag * inverse_imag
                value_imag = numer_real * inverse_imag + numer_imag * inverse_real
            return value_real, value_imag

        solution_real, solution_imag = lax.map(solve_mode, (spectrum_real, spectrum_imag, shift_real, shift_imag))
        update = jnp.real(jnp.fft.ifft(solution_real, axis=0)) - jnp.imag(jnp.fft.ifft(solution_imag, axis=0))
        thickness = thickness - update / weight_up[:, None, None]
    return thickness
```

```python
import functools
import math

import jax
import jax.numpy as jnp
from jax import lax
from jax.experimental import pallas as pl
from jax.experimental.pallas import tpu as pltpu
from jax.sharding import PartitionSpec as P

NEWTON = 2
SWEEPS = 8
HALO = NEWTON * SWEEPS
SUB = 8

circulant_weight = 0.25
time_step = 1.0


vmem = pl.BlockSpec(memory_space=pltpu.VMEM)
params = pltpu.CompilerParams(vmem_limit_bytes=16 * 1024 * 1024)


def struct(*shape):
    return jax.ShapeDtypeStruct(shape, jnp.float32)


def pack_kernel(levels, strip, edge_count, *refs):
    guess, balance, start, bed, rate, flags = refs[:6]
    strips = refs[6 : 6 + levels]
    edges = refs[6 + levels : 6 + 2 * levels]
    fixed = refs[6 + 2 * levels]
    wide = refs[-1]
    rows = guess.shape[1]
    high = strip + 2 * HALO
    me = lax.axis_index("tm")
    boost = jnp.where(flags[...] == 2, 2.0, 1.0)
    ice = jnp.where(flags[...] != 0, boost * rate[...], 0.0)
    for index, part in enumerate((guess[0], balance[0], start[...], bed[...], ice)):
        wide[index, :HALO] = jnp.zeros((HALO, part.shape[1]), jnp.float32)
        wide[index, HALO : HALO + rows] = part
        wide[index, HALO + rows :] = jnp.zeros((HALO, part.shape[1]), jnp.float32)
    for shift in range(levels):
        target = lax.rem(me + shift, levels)
        strips[shift][...] = wide[:2, pl.ds(pl.multiple_of(target * strip, SUB), high)]
        first = jnp.where(target < edge_count, rows, HALO)
        count = edges[shift].shape[0]
        edges[shift][...] = wide[:count, pl.ds(pl.multiple_of(first, SUB), HALO)]
    fixed[...] = wide[2:, pl.ds(pl.multiple_of(me * strip, SUB), high)]


def join_kernel(levels, strip, edge_count, *refs):
    strips = refs[:levels]
    edges = refs[levels : 2 * levels]
    fixed = refs[2 * levels]
    out = refs[-1]
    high = strip + 2 * HALO
    me = lax.axis_index("tm")
    out[2 * levels :] = fixed[...]
    for shift in range(levels):
        level = lax.rem(me + levels - shift, levels)
        out[level] = strips[shift][0]
        out[levels + level] = strips[shift][1]

    def overlay(here, there):
        for shift in range(levels):
            level = lax.rem(me + levels - shift, levels)
            out[level, here] = edges[shift][0, there]
            out[levels + level, here] = edges[shift][1, there]
        out[2 * levels :, here] = edges[0][2:, there]

    for place in range(edge_count):
        count = HALO - strip * place

        @pl.when(me == place)
        def _():
            overlay(slice(0, count), slice(HALO - count, HALO))

        @pl.when(me == levels - 1 - place)
        def _():
            overlay(slice(high - count, high), slice(0, count))


def mode_fields(levels):
    fields, count = [], 0
    for mode in range(levels // 2 + 1):
        if 2 * mode % levels == 0:
            fields.append((mode, count, None))
            count += 1
        else:
            fields.append((mode, count, count + 1))
            count += 2
    return fields, count


def wave(levels, product):
    product %= levels
    quarter = 4 * product
    if quarter % levels == 0:
        return ((1.0, 0.0), (0.0, 1.0), (-1.0, 0.0), (0.0, -1.0))[quarter // levels]
    angle = 2.0 * math.pi * product / levels
    return math.cos(angle), math.sin(angle)


def combine(terms):
    total = None
    for coeff, value in terms:
        if coeff == 0.0:
            continue
        if total is None:
            total = value if coeff == 1.0 else coeff * value
        elif coeff == 1.0:
            total = total + value
        elif coeff == -1.0:
            total = total - value
        else:
            total = total + coeff * value
    return total


def newton_kernel(levels, parts, strip, *refs):
    blocks = refs[:parts]
    outs = refs[parts : parts + levels]
    height, balance, fixed, diff, weight, inverse, source, value, plain = refs[parts + levels :]
    high, width = blocks[0].shape[1:]
    depth = high // SUB
    across = parts * width
    me = lax.axis_index("tm")
    column = lax.axis_index("sy") * width
    lane = lax.broadcasted_iota(jnp.int32, (SUB, across), 1)
    first = lane == lax.rem(across - column, across)
    last = lane == across - 1 - column
    fields, field_count = mode_fields(levels)
    root = circulant_weight ** (1.0 / levels)

    def from_left(array):
        return pltpu.roll(array, 1, axis=1)

    def from_right(array):
        return pltpu.roll(array, across - 1, axis=1)

    def from_above(array):
        return pltpu.roll(array, 1, axis=0)

    def from_below(array):
        return pltpu.roll(array, SUB - 1, axis=0)

    def spread(field, q):
        return jnp.concatenate([block[field, pl.ds(q, SUB, stride=depth), :] for block in blocks], axis=1)

    for q in range(depth):
        for level in range(levels):
            height[level, q] = spread(level, q)
            balance[level, q] = spread(levels + level, q)
        for index in range(3):
            fixed[index, q] = spread(2 * levels + index, q)

    def newton(step, carry):
        for q in range(depth):
            ice = fixed[2, q]
            total = None
            for level in range(levels):
                thick = height[level, q]
                diffuse = ice * thick * thick * jnp.abs(thick)
                diff[level, q] = diffuse
                total = diffuse if total is None else total + diffuse
            weight[4, q] = total * (0.5 / levels)
        half = [weight[4, q] for q in range(depth)]
        downs = [half[q] + (half[q + 1] if q + 1 < depth else from_below(half[0])) for q in range(depth)]
        for q in range(depth):
            down = downs[q]
            up = downs[q - 1] if q > 0 else from_above(downs[depth - 1])
            right = half[q] + jnp.where(last, 0.0, from_right(half[q]))
            left = half[q] + jnp.where(first, 0.0, from_left(half[q]))
            weight[0, q] = up
            weight[1, q] = down
            weight[2, q] = jnp.where(first, 0.0, left)
            weight[3, q] = jnp.where(last, 0.0, right)
            total = up + down + left + right
            inside = jnp.where(fixed[2, q] > 0.0, 1.0, 0.0)
            for mode, real, imag in fields:
                cosine, sine = wave(levels, mode)
                denom = total + (1.0 - root * cosine) / time_step
                if imag is None:
                    inverse[real, q] = inside / denom
                else:
                    shift = root * sine / time_step
                    ratio = inside / (denom * denom + shift * shift)
                    inverse[real, q] = ratio * denom
                    inverse[imag, q] = ratio * -shift
        for level in range(levels):
            def surface_at(q):
                return height[level, q] + fixed[1, q]

            def flux(d0, s0, d1, s1):
                return (d0 + d1) * (s0 - s1)

            d_last, s_last = diff[level, depth - 1], surface_at(depth - 1)
            d_here, s_here = diff[level, 0], surface_at(0)
            d_wrap, s_wrap = from_below(d_here), from_below(s_here)
            above = from_above(flux(d_last, s_last, d_wrap, s_wrap))
            for q in range(depth):
                if q + 1 < depth:
                    d_next, s_next = diff[level, q + 1], surface_at(q + 1)
                else:
                    d_next, s_next = d_wrap, s_wrap
                below = flux(d_here, s_here, d_next, s_next)
                right = flux(
                    d_here, s_here,
                    jnp.where(last, 0.0, from_right(d_here)), jnp.where(last, 0.0, from_right(s_here)),
                )
                left = jnp.where(first, d_here * s_here, -from_left(right))
                prior = height[level - 1, q] if level > 0 else fixed[0, q]
                change = (
                    (height[level, q] - prior) / time_step
                    + 0.5 * ((below - above) + (right + left))
                    - balance[level, q]
                )
                scaled = change if level == 0 else change * root**level
                diff[level, q] = jnp.where(fixed[2, q] > 0.0, scaled, 0.0)
                above, d_here, s_here = below, d_next, s_next
        for q in range(depth):
            scaled = [diff[level, q] for level in range(levels)]
            for mode, real, imag in fields:
                waves = [wave(levels, mode * level) for level in range(levels)]
                y_real = combine([(w[0], v) for w, v in zip(waves, scaled)])
                source[real, q] = y_real
                if imag is None:
                    value[real, q] = inverse[real, q] * y_real
                else:
                    y_imag = combine([(-w[1], v) for w, v in zip(waves, scaled)])
                    source[imag, q] = y_imag
                    i_real, i_imag = inverse[real, q], inverse[imag, q]
                    value[real, q] = y_real * i_real - y_imag * i_imag
                    value[imag, q] = y_real * i_imag + y_imag * i_real

        def sweep(index, carry):
            tops = [value[f, 0] for f in range(field_count)]
            befores = [from_above(value[f, depth - 1]) for f in range(field_count)]
            heres = tops
            for q in range(depth):
                up, down, left, right = (weight[i, q] for i in range(4))
                nexts, numer = [], []
                for f in range(field_count):
                    after = value[f, q + 1] if q + 1 < depth else from_below(tops[f])
                    nexts.append(after)
                    numer.append(
                        source[f, q]
                        + ((up * befores[f] + down * after)
                        + (left * from_left(heres[f]) + right * from_right(heres[f])))
                    )
                for mode, real, imag in fields:
                    if imag is None:
                        value[real, q] = inverse[real, q] * numer[real]
                    else:
                        i_real, i_imag = inverse[real, q], inverse[imag, q]
                        value[real, q] = numer[real] * i_real - numer[imag] * i_imag
                        value[imag, q] = numer[real] * i_imag + numer[imag] * i_real
                befores, heres = heres, nexts
            return carry

        lax.fori_loop(0, SWEEPS - 1, sweep, 0)
        for q in range(depth):
            for level in range(levels):
                scale = 1.0 / (levels * root**level)
                terms = []
                for mode, real, imag in fields:
                    cosine, sine = wave(levels, mode * level)
                    if imag is None:
                        terms.append((-scale * cosine, value[real, q]))
                    else:
                        terms.append((-2.0 * scale * cosine, value[real, q]))
                        terms.append((2.0 * scale * sine, value[imag, q]))
                height[level, q] = height[level, q] + combine(terms)
        return carry

    lax.fori_loop(0, NEWTON, newton, 0)
    for level in range(levels):
        for q in range(depth):
            plain[level, pl.ds(q, SUB, stride=depth), :] = height[level, q, :, :width]
    for shift in range(levels):
        target = lax.rem(me + shift, levels)
        outs[shift][...] = plain[target, HALO : HALO + strip]


def place_kernel(levels, strip, *refs):
    out = refs[-1]
    me = lax.axis_index("tm")
    for shift in range(levels):
        origin = lax.rem(me + levels - shift, levels)
        out[0, pl.ds(pl.multiple_of(origin * strip, SUB), strip)] = refs[shift][...]


def body(sizes, thickness_guess, thickness_start, bed, rate_factor, mass_balance, cell_flags):
    levels, tiles, parts = sizes
    rows, cols = thickness_start.shape
    strip = rows // levels
    high = strip + 2 * HALO
    edge_count = -(-HALO // strip)
    count = 2 * levels + 3
    _, field_count = mode_fields(levels)
    depth = high // SUB

    packed = pl.pallas_call(
        functools.partial(pack_kernel, levels, strip, edge_count),
        out_shape=[struct(2, high, cols)] * levels
        + [struct(5 if shift == 0 else 2, HALO, cols) for shift in range(levels)]
        + [struct(3, high, cols)],
        in_specs=[vmem] * 6,
        out_specs=[vmem] * (2 * levels + 1),
        scratch_shapes=[pltpu.VMEM((5, rows + 2 * HALO, cols), jnp.float32)],
        compiler_params=params,
        name="pack",
    )(thickness_guess, mass_balance, thickness_start, bed, rate_factor, cell_flags)
    strips, edges, fixed = packed[:levels], packed[levels : 2 * levels], packed[-1]

    def around(value, shift):
        return lax.ppermute(value, "tm", [(i, (i + shift) % levels) for i in range(levels)])

    def device(tm, sx, sy):
        return (tm * tiles + sx) * parts + sy

    def edge_pairs(shift):
        pairs = []
        for level in range(levels):
            target = (level + shift) % levels
            for tile in range(tiles):
                if target < edge_count:
                    other = tile + 1
                elif target >= levels - edge_count:
                    other = tile - 1
                else:
                    continue
                if 0 <= other < tiles:
                    pairs += [(device(level, tile, part), device(target, other, part)) for part in range(parts)]
        return pairs

    strips = [strips[0]] + [around(strips[shift], shift) for shift in range(1, levels)]
    edges = [lax.ppermute(edges[shift], ("tm", "sx", "sy"), edge_pairs(shift)) for shift in range(levels)]
    mine = pl.pallas_call(
        functools.partial(join_kernel, levels, strip, edge_count),
        out_shape=struct(count, high, cols),
        in_specs=[vmem] * (2 * levels + 1),
        out_specs=vmem,
        compiler_params=params,
        name="join",
    )(*strips, *edges, fixed)
    others = [
        lax.ppermute(mine, "sy", [(i, (i - shift) % parts) for i in range(parts)])
        for shift in range(1, parts)
    ]
    across = parts * cols
    pieces = pl.pallas_call(
        functools.partial(newton_kernel, levels, parts, strip),
        out_shape=[struct(strip, cols)] * levels,
        in_specs=[vmem] * parts,
        out_specs=[vmem] * levels,
        scratch_shapes=[
            pltpu.VMEM(shape, jnp.float32)
            for shape in (
                (levels, depth, SUB, across),
                (levels, depth, SUB, across),
                (3, depth, SUB, across),
                (levels, depth, SUB, across),
                (5, depth, SUB, across),
                (field_count, depth, SUB, across),
                (field_count, depth, SUB, across),
                (field_count, depth, SUB, across),
                (levels, high, cols),
            )
        ],
        compiler_params=params,
        name="newton",
    )(mine, *others)
    pieces = [pieces[0]] + [around(pieces[shift], shift) for shift in range(1, levels)]
    return pl.pallas_call(
        functools.partial(place_kernel, levels, strip),
        out_shape=struct(1, rows, cols),
        in_specs=[vmem] * levels,
        out_specs=vmem,
        compiler_params=params,
        name="place",
    )(*pieces)


def solution(mesh):
    sizes = tuple(mesh.shape[axis] for axis in ("tm", "sx", "sy"))
    in_specs = (
        P("tm", "sx", "sy"),
        P("sx", "sy"),
        P("sx", "sy"),
        P("sx", "sy"),
        P("tm", "sx", "sy"),
        P("sx", "sy"),
    )
    out_specs = P("tm", "sx", "sy")
    return jax.shard_map(
        functools.partial(body, sizes), mesh=mesh, in_specs=in_specs, out_specs=out_specs, check_vma=False
    )
```

```python
import functools
import math

import jax
import jax.numpy as jnp
from jax import lax
from jax.experimental import pallas as pl
from jax.experimental.pallas import tpu as pltpu
from jax.sharding import PartitionSpec as P

NEWTON = 2
SWEEPS = 8
HALO = NEWTON * SWEEPS
SUB = 8

circulant_weight = 0.25
time_step = 1.0


vmem = pl.BlockSpec(memory_space=pltpu.VMEM)
params = pltpu.CompilerParams(vmem_limit_bytes=16 * 1024 * 1024)


def struct(*shape):
    return jax.ShapeDtypeStruct(shape, jnp.float32)


def strip_of(levels, tm):
    return jnp.where(lax.rem(lax.axis_index("sx"), 2) == 0, tm, levels - 1 - tm)


def pack_kernel(levels, strip, *refs):
    guess, balance, start, bed, rate, flags = refs[:6]
    strips = refs[6 : 6 + levels]
    fixed, ice, kind, sems = refs[6 + levels :]
    me = lax.axis_index("tm")

    def rows_of(tm):
        return pl.ds(pl.multiple_of(strip_of(levels, tm) * strip, SUB), strip)

    copies = []
    for shift in range(levels):
        here = rows_of(lax.rem(me + shift, levels))
        copies += [(guess.at[0, here], strips[shift].at[0]), (balance.at[0, here], strips[shift].at[1])]
    here = rows_of(me)
    copies += [
        (start.at[here], fixed.at[0]),
        (bed.at[here], fixed.at[1]),
        (rate.at[here], ice),
        (flags.at[here], kind),
    ]
    copies = [pltpu.make_async_copy(a, b, sems.at[i]) for i, (a, b) in enumerate(copies)]
    for copy in copies:
        copy.start()
    for copy in copies:
        copy.wait()
    boost = jnp.where(kind[...] == 2, 2.0, 1.0)
    fixed[2] = jnp.where(kind[...] != 0, boost * ice[...], 0.0)


def rim_kernel(levels, counts, *refs):
    strips = refs[:levels]
    fixed = refs[levels]
    lows, highs = refs[levels + 1 : levels + 1 + len(counts)], refs[levels + 1 + len(counts) :]
    me = lax.axis_index("tm")
    strip = fixed.shape[1]
    for count, low, high in zip(counts, lows, highs):
        for out, rows in ((low, slice(0, count)), (high, slice(strip - count, strip))):
            for shift in range(levels):
                level = lax.rem(me + levels - shift, levels)
                out[level] = strips[shift][0, rows]
                out[levels + level] = strips[shift][1, rows]
            out[2 * levels :] = fixed[:, rows]


def join_kernel(levels, counts, *refs):
    strips = refs[:levels]
    fixed = refs[levels]
    aboves, belows = refs[levels + 1 : levels + 1 + len(counts)], refs[levels + 1 + len(counts) : -1]
    out = refs[-1]
    me = lax.axis_index("tm")
    strip = fixed.shape[1]
    middle = slice(HALO, HALO + strip)
    for shift in range(levels):
        level = lax.rem(me + levels - shift, levels)
        out[level, middle] = strips[shift][0]
        out[levels + level, middle] = strips[shift][1]
    out[2 * levels :, middle] = fixed[...]
    done = 0
    for count, above, below in zip(counts, aboves, belows):
        out[:, HALO - done - count : HALO - done] = above[...]
        out[:, HALO + strip + done : HALO + strip + done + count] = below[...]
        done += count


def mode_fields(levels):
    fields, count = [], 0
    for mode in range(levels // 2 + 1):
        if 2 * mode % levels == 0:
            fields.append((mode, count, None))
            count += 1
        else:
            fields.append((mode, count, count + 1))
            count += 2
    return fields, count


def wave(levels, product):
    product %= levels
    quarter = 4 * product
    if quarter % levels == 0:
        return ((1.0, 0.0), (0.0, 1.0), (-1.0, 0.0), (0.0, -1.0))[quarter // levels]
    angle = 2.0 * math.pi * product / levels
    return math.cos(angle), math.sin(angle)


def combine(terms):
    total = None
    for coeff, value in terms:
        if coeff == 0.0:
            continue
        if total is None:
            total = value if coeff == 1.0 else coeff * value
        elif coeff == 1.0:
            total = total + value
        elif coeff == -1.0:
            total = total - value
        else:
            total = total + coeff * value
    return total


def newton_kernel(levels, parts, strip, *refs):
    blocks = refs[:parts]
    outs = refs[parts : parts + levels]
    height, balance, fixed, diff, weight, inverse, source, value, plain = refs[parts + levels :]
    high, width = blocks[0].shape[1:]
    depth = high // SUB
    across = parts * width
    me = lax.axis_index("tm")
    column = lax.axis_index("sy") * width
    lane = lax.broadcasted_iota(jnp.int32, (SUB, across), 1)
    first = lane == lax.rem(across - column, across)
    last = lane == across - 1 - column
    fields, field_count = mode_fields(levels)
    root = circulant_weight ** (1.0 / levels)

    def from_left(array):
        return pltpu.roll(array, 1, axis=1)

    def from_right(array):
        return pltpu.roll(array, across - 1, axis=1)

    def from_above(array):
        return pltpu.roll(array, 1, axis=0)

    def from_below(array):
        return pltpu.roll(array, SUB - 1, axis=0)

    def spread(field, q):
        return jnp.concatenate([block[field, pl.ds(q, SUB, stride=depth), :] for block in blocks], axis=1)

    for q in range(depth):
        for level in range(levels):
            height[level, q] = spread(level, q)
            balance[level, q] = spread(levels + level, q)
        for index in range(3):
            fixed[index, q] = spread(2 * levels + index, q)

    def newton(step, carry):
        for q in range(depth):
            ice = fixed[2, q]
            total = None
            for level in range(levels):
                thick = height[level, q]
                diffuse = ice * thick * thick * jnp.abs(thick)
                diff[level, q] = diffuse
                total = diffuse if total is None else total + diffuse
            weight[4, q] = total * (0.5 / levels)
        half = [weight[4, q] for q in range(depth)]
        downs = [half[q] + (half[q + 1] if q + 1 < depth else from_below(half[0])) for q in range(depth)]
        for q in range(depth):
            down = downs[q]
            up = downs[q - 1] if q > 0 else from_above(downs[depth - 1])
            right = half[q] + jnp.where(last, 0.0, from_right(half[q]))
            left = half[q] + jnp.where(first, 0.0, from_left(half[q]))
            weight[0, q] = up
            weight[1, q] = down
            weight[2, q] = jnp.where(first, 0.0, left)
            weight[3, q] = jnp.where(last, 0.0, right)
            total = up + down + left + right
            inside = jnp.where(fixed[2, q] > 0.0, 1.0, 0.0)
            for mode, real, imag in fields:
                cosine, sine = wave(levels, mode)
                denom = total + (1.0 - root * cosine) / time_step
                if imag is None:
                    inverse[real, q] = inside / denom
                else:
                    shift = root * sine / time_step
                    ratio = inside / (denom * denom + shift * shift)
                    inverse[real, q] = ratio * denom
                    inverse[imag, q] = ratio * -shift
        for level in range(levels):
            def surface_at(q):
                return height[level, q] + fixed[1, q]

            def flux(d0, s0, d1, s1):
                return (d0 + d1) * (s0 - s1)

            d_last, s_last = diff[level, depth - 1], surface_at(depth - 1)
            d_here, s_here = diff[level, 0], surface_at(0)
            d_wrap, s_wrap = from_below(d_here), from_below(s_here)
            above = from_above(flux(d_last, s_last, d_wrap, s_wrap))
            for q in range(depth):
                if q + 1 < depth:
                    d_next, s_next = diff[level, q + 1], surface_at(q + 1)
                else:
                    d_next, s_next = d_wrap, s_wrap
                below = flux(d_here, s_here, d_next, s_next)
                right = flux(
                    d_here, s_here,
                    jnp.where(last, 0.0, from_right(d_here)), jnp.where(last, 0.0, from_right(s_here)),
                )
                left = jnp.where(first, d_here * s_here, -from_left(right))
                prior = height[level - 1, q] if level > 0 else fixed[0, q]
                change = (
                    (height[level, q] - prior) / time_step
                    + 0.5 * ((below - above) + (right + left))
                    - balance[level, q]
                )
                scaled = change if level == 0 else change * root**level
                diff[level, q] = jnp.where(fixed[2, q] > 0.0, scaled, 0.0)
                above, d_here, s_here = below, d_next, s_next
        for q in range(depth):
            scaled = [diff[level, q] for level in range(levels)]
            for mode, real, imag in fields:
                waves = [wave(levels, mode * level) for level in range(levels)]
                y_real = combine([(w[0], v) for w, v in zip(waves, scaled)])
                source[real, q] = y_real
                if imag is None:
                    value[real, q] = inverse[real, q] * y_real
                else:
                    y_imag = combine([(-w[1], v) for w, v in zip(waves, scaled)])
                    source[imag, q] = y_imag
                    i_real, i_imag = inverse[real, q], inverse[imag, q]
                    value[real, q] = y_real * i_real - y_imag * i_imag
                    value[imag, q] = y_real * i_imag + y_imag * i_real

        def sweep(index, carry):
            tops = [value[f, 0] for f in range(field_count)]
            befores = [from_above(value[f, depth - 1]) for f in range(field_count)]
            heres = tops
            for q in range(depth):
                up, down, left, right = (weight[i, q] for i in range(4))
                nexts, numer = [], []
                for f in range(field_count):
                    after = value[f, q + 1] if q + 1 < depth else from_below(tops[f])
                    nexts.append(after)
                    numer.append(
                        source[f, q]
                        + ((up * befores[f] + down * after)
                        + (left * from_left(heres[f]) + right * from_right(heres[f])))
                    )
                for mode, real, imag in fields:
                    if imag is None:
                        value[real, q] = inverse[real, q] * numer[real]
                    else:
                        i_real, i_imag = inverse[real, q], inverse[imag, q]
                        value[real, q] = numer[real] * i_real - numer[imag] * i_imag
                        value[imag, q] = numer[real] * i_imag + numer[imag] * i_real
                befores, heres = heres, nexts
            return carry

        lax.fori_loop(0, SWEEPS - 1, sweep, 0)
        for q in range(depth):
            for level in range(levels):
                scale = 1.0 / (levels * root**level)
                terms = []
                for mode, real, imag in fields:
                    cosine, sine = wave(levels, mode * level)
                    if imag is None:
                        terms.append((-scale * cosine, value[real, q]))
                    else:
                        terms.append((-2.0 * scale * cosine, value[real, q]))
                        terms.append((2.0 * scale * sine, value[imag, q]))
                height[level, q] = height[level, q] + combine(terms)
        return carry

    lax.fori_loop(0, NEWTON, newton, 0)
    for level in range(levels):
        for q in range(depth):
            plain[level, pl.ds(q, SUB, stride=depth), :] = height[level, q, :, :width]
    for shift in range(levels):
        target = lax.rem(me + shift, levels)
        outs[shift][...] = plain[target, HALO : HALO + strip]


def place_kernel(levels, strip, *refs):
    out = refs[-1]
    me = lax.axis_index("tm")
    for shift in range(levels):
        origin = strip_of(levels, lax.rem(me + levels - shift, levels))
        out[0, pl.ds(pl.multiple_of(origin * strip, SUB), strip)] = refs[shift][...]


def body(sizes, thickness_guess, thickness_start, bed, rate_factor, mass_balance, cell_flags):
    levels, tiles, parts = sizes
    rows, cols = thickness_start.shape
    strip = rows // levels
    high = strip + 2 * HALO
    count = 2 * levels + 3
    _, field_count = mode_fields(levels)
    depth = high // SUB
    across = parts * cols
    counts = [min(strip, HALO - done) for done in range(0, HALO, strip)]

    packed = pl.pallas_call(
        functools.partial(pack_kernel, levels, strip),
        out_shape=[struct(2, strip, cols)] * levels + [struct(3, strip, cols)],
        in_specs=[pl.BlockSpec(memory_space=pl.ANY)] * 6,
        out_specs=[vmem] * (levels + 1),
        scratch_shapes=[
            pltpu.VMEM((strip, cols), jnp.float32),
            pltpu.VMEM((strip, cols), jnp.int32),
            pltpu.SemaphoreType.DMA((2 * levels + 4,)),
        ],
        compiler_params=params,
        name="pack",
    )(thickness_guess, mass_balance, thickness_start, bed, rate_factor, cell_flags)
    strips, fixed = packed[:levels], packed[levels]

    def around(value, shift):
        return lax.ppermute(value, "tm", [(i, (i + shift) % levels) for i in range(levels)])

    snake = [
        (tm if tile % 2 == 0 else levels - 1 - tm, tile) for tile in range(tiles) for tm in range(levels)
    ]

    def along(value, hops):
        pairs = []
        for place, (tm, tile) in enumerate(snake):
            if 0 <= place + hops < len(snake):
                other_tm, other_tile = snake[place + hops]
                pairs += [
                    ((tm * tiles + tile) * parts + part, (other_tm * tiles + other_tile) * parts + part)
                    for part in range(parts)
                ]
        return lax.ppermute(value, ("tm", "sx", "sy"), pairs)

    strips = [strips[0]] + [around(strips[shift], shift) for shift in range(1, levels)]
    rims = pl.pallas_call(
        functools.partial(rim_kernel, levels, counts),
        out_shape=[struct(count, n, cols) for n in counts] * 2,
        in_specs=[vmem] * (levels + 1),
        out_specs=[vmem] * (2 * len(counts)),
        compiler_params=params,
        name="rim",
    )(*strips, fixed)
    aboves = [along(rims[len(counts) + i], i + 1) for i in range(len(counts))]
    belows = [along(rims[i], -(i + 1)) for i in range(len(counts))]
    mine = pl.pallas_call(
        functools.partial(join_kernel, levels, counts),
        out_shape=struct(count, high, cols),
        in_specs=[vmem] * (levels + 1 + 2 * len(counts)),
        out_specs=vmem,
        compiler_params=params,
        name="join",
    )(*strips, fixed, *aboves, *belows)
    others = [
        lax.ppermute(mine, "sy", [(i, (i - shift) % parts) for i in range(parts)])
        for shift in range(1, parts)
    ]
    pieces = pl.pallas_call(
        functools.partial(newton_kernel, levels, parts, strip),
        out_shape=[struct(strip, cols)] * levels,
        in_specs=[vmem] * parts,
        out_specs=[vmem] * levels,
        scratch_shapes=[
            pltpu.VMEM(shape, jnp.float32)
            for shape in (
                (levels, depth, SUB, across),
                (levels, depth, SUB, across),
                (3, depth, SUB, across),
                (levels, depth, SUB, across),
                (5, depth, SUB, across),
                (field_count, depth, SUB, across),
                (field_count, depth, SUB, across),
                (field_count, depth, SUB, across),
                (levels, high, cols),
            )
        ],
        compiler_params=params,
        name="newton",
    )(mine, *others)
    pieces = [pieces[0]] + [around(pieces[shift], shift) for shift in range(1, levels)]
    return pl.pallas_call(
        functools.partial(place_kernel, levels, strip),
        out_shape=struct(1, rows, cols),
        in_specs=[vmem] * levels,
        out_specs=vmem,
        compiler_params=params,
        name="place",
    )(*pieces)


def solution(mesh):
    sizes = tuple(mesh.shape[axis] for axis in ("tm", "sx", "sy"))
    in_specs = (
        P("tm", "sx", "sy"),
        P("sx", "sy"),
        P("sx", "sy"),
        P("sx", "sy"),
        P("tm", "sx", "sy"),
        P("sx", "sy"),
    )
    out_specs = P("tm", "sx", "sy")
    return jax.shard_map(
        functools.partial(body, sizes), mesh=mesh, in_specs=in_specs, out_specs=out_specs, check_vma=False
    )
```

```python
import functools
import math

import jax
import jax.numpy as jnp
from jax import lax
from jax.experimental import pallas as pl
from jax.experimental.pallas import tpu as pltpu
from jax.sharding import PartitionSpec as P

NEWTON = 2
SWEEPS = 8
HALO = NEWTON * SWEEPS
SUB = 8

circulant_weight = 0.25
time_step = 1.0


vmem = pl.BlockSpec(memory_space=pltpu.VMEM)
hbm = pl.BlockSpec(memory_space=pltpu.HBM)
params = pltpu.CompilerParams(vmem_limit_bytes=16 * 1024 * 1024)


def struct(*shape):
    return jax.ShapeDtypeStruct(shape, jnp.float32)


def aligned(index):
    return pl.multiple_of(index, SUB)


def strip_of(levels, tm):
    return jnp.where(lax.rem(lax.axis_index("sx"), 2) == 0, tm, levels - 1 - tm)


def level_of(levels, shift):
    return lax.rem(lax.axis_index("tm") + levels - shift, levels)


def pack_kernel(levels, strip, *refs):
    guess, balance, start, bed, rate, flags = refs[:6]
    strips = refs[6 : 6 + levels]
    fixed, ice, kind, sems = refs[6 + levels :]
    me = lax.axis_index("tm")

    def rows_of(tm):
        return pl.ds(aligned(strip_of(levels, tm) * strip), strip)

    copies = []
    for shift in range(levels):
        here = rows_of(lax.rem(me + shift, levels))
        copies += [(guess.at[0, here], strips[shift].at[0]), (balance.at[0, here], strips[shift].at[1])]
    here = rows_of(me)
    copies += [
        (start.at[here], fixed.at[0]),
        (bed.at[here], fixed.at[1]),
        (rate.at[here], ice),
        (flags.at[here], kind),
    ]
    copies = [pltpu.make_async_copy(a, b, sems.at[i]) for i, (a, b) in enumerate(copies)]
    for copy in copies:
        copy.start()
    for copy in copies:
        copy.wait()
    boost = jnp.where(kind[...] == 2, 2.0, 1.0)
    fixed[2] = jnp.where(kind[...] != 0, boost * ice[...], 0.0)


def lay(levels, out, rows, strips, fixed, source):
    for shift in range(levels):
        level = level_of(levels, shift)
        out[level, rows] = strips[shift][0, source]
        out[levels + level, rows] = strips[shift][1, source]
    out[2 * levels :, rows] = fixed[:, source]


def give_kernel(levels, keep, *refs):
    strips, fixed, out = refs[:levels], refs[levels], refs[-1]
    strip = fixed.shape[1]
    first = aligned((1 - lax.axis_index("sy")) * (strip - keep))
    lay(levels, out, slice(0, keep), strips, fixed, pl.ds(first, keep))


def edge_kernel(levels, *refs):
    strips, fixed, take, out = refs[:levels], refs[levels], refs[levels + 1], refs[-1]
    strip, keep = fixed.shape[1], take.shape[1]
    part = lax.axis_index("sy")
    out[:, 0] = take[:, pl.ds(aligned(part * (keep - HALO)), HALO)]
    source = pl.ds(aligned(part * (strip - HALO)), HALO)
    for shift in range(levels):
        level = level_of(levels, shift)
        out[level, 1] = strips[shift][0, source]
        out[levels + level, 1] = strips[shift][1, source]
    out[2 * levels :, 1] = fixed[:, source]


def rim_kernel(levels, counts, *refs):
    strips = refs[:levels]
    fixed = refs[levels]
    lows, highs = refs[levels + 1 : levels + 1 + len(counts)], refs[levels + 1 + len(counts) :]
    strip = fixed.shape[1]
    for count, low, high in zip(counts, lows, highs):
        lay(levels, low, slice(0, count), strips, fixed, slice(0, count))
        lay(levels, high, slice(0, count), strips, fixed, slice(strip - count, strip))


def join_kernel(levels, counts, *refs):
    strips = refs[:levels]
    fixed = refs[levels]
    aboves, belows = refs[levels + 1 : levels + 1 + len(counts)], refs[levels + 1 + len(counts) : -1]
    out = refs[-1]
    strip = fixed.shape[1]
    lay(levels, out, slice(HALO, HALO + strip), strips, fixed, slice(0, strip))
    done = 0
    for count, above, below in zip(counts, aboves, belows):
        out[:, HALO - done - count : HALO - done] = above[...]
        out[:, HALO + strip + done : HALO + strip + done + count] = below[...]
        done += count


def mode_fields(levels):
    fields, count = [], 0
    for mode in range(levels // 2 + 1):
        if 2 * mode % levels == 0:
            fields.append((mode, count, None))
            count += 1
        else:
            fields.append((mode, count, count + 1))
            count += 2
    return fields, count


def wave(levels, product):
    product %= levels
    quarter = 4 * product
    if quarter % levels == 0:
        return ((1.0, 0.0), (0.0, 1.0), (-1.0, 0.0), (0.0, -1.0))[quarter // levels]
    angle = 2.0 * math.pi * product / levels
    return math.cos(angle), math.sin(angle)


def combine(terms):
    total = None
    for coeff, value in terms:
        if coeff == 0.0:
            continue
        if total is None:
            total = value if coeff == 1.0 else coeff * value
        elif coeff == 1.0:
            total = total + value
        elif coeff == -1.0:
            total = total - value
        else:
            total = total + coeff * value
    return total


def pick(array, index):
    return jnp.take_along_axis(array, index, axis=1, mode="promise_in_bounds")


def scratches(levels, depth, cols, high):
    _, field_count = mode_fields(levels)
    shapes = [(count, depth, 2, SUB, cols) for count in (levels, levels, 3, levels, 5, *(field_count,) * 4)]
    shapes.append((4, levels, depth, SUB, cols))
    shapes.append((levels, 2, high, cols))
    return [pltpu.VMEM(shape, jnp.float32) for shape in shapes]


def newton_steps(levels, load, spaces):
    height, balance, fixed, diff, weight, inverse, source, value, side, sides, plain = spaces
    depth, _, _, cols = height.shape[1:]
    across = 2 * cols
    lane = lax.broadcasted_iota(jnp.int32, (SUB, cols), 1)
    low = lane < cols // 2
    column = lax.axis_index("sy") * cols
    first = 2 * lane == lax.rem(across - column, across)
    last = 2 * lane + 1 == across - 1 - column
    parting = jnp.where(low, 2 * lane, 2 * lane - (cols - 1))
    mixing = (lane // 2) + (lane % 2) * (cols // 2)
    fields, field_count = mode_fields(levels)
    root = circulant_weight ** (1.0 / levels)

    def half_turn(array):
        return pltpu.roll(array, cols // 2, axis=1)

    def before(odd):
        return pltpu.roll(odd, 1, axis=1)

    def after(even):
        return pltpu.roll(even, cols - 1, axis=1)

    def from_above(array):
        return pltpu.roll(array, 1, axis=0)

    def from_below(array):
        return pltpu.roll(array, SUB - 1, axis=0)

    def rows_around(read):
        blocks = [read(q) for q in range(depth)]
        return [from_above(blocks[-1])] + blocks + [from_below(blocks[0])]

    places = [(height, level, level) for level in range(levels)]
    places += [(balance, level, levels + level) for level in range(levels)]
    places += [(fixed, index, 2 * levels + index) for index in range(3)]
    for ref, index, field in places:
        for q in range(depth):
            left, right = (pick(load(field, half, q), parting) for half in range(2))
            ref[index, q, 0] = jnp.where(low, left, half_turn(right))
            ref[index, q, 1] = jnp.where(low, half_turn(left), right)

    def newton(step, carry):
        for q in range(depth):
            totals = [None] * 4
            for level in range(levels):
                thick = [height[level, q, r] for r in range(2)]
                d = [fixed[2, q, r] * thick[r] * thick[r] * jnp.abs(thick[r]) for r in range(2)]
                s = [thick[r] + fixed[1, q, r] for r in range(2)]
                for r in range(2):
                    diff[level, q, r] = d[r]
                d_left, d_right = jnp.where(first, 0.0, before(d[1])), jnp.where(last, 0.0, after(d[0]))
                sides[0, level, q] = d_left
                sides[1, level, q] = d_right
                sides[2, level, q] = jnp.where(first, 0.0, before(s[1]))
                sides[3, level, q] = jnp.where(last, 0.0, after(s[0]))
                for i, part in enumerate((d[0], d[1], d_left, d_right)):
                    totals[i] = part if level == 0 else totals[i] + part
            even, odd, left, right = (total * (0.5 / levels) for total in totals)
            weight[0, q, 0], weight[0, q, 1] = even, odd
            weight[4, q, 0], weight[4, q, 1] = left, right
        for r in range(2):
            halves = rows_around(lambda q: weight[0, q, r])
            downs = [halves[q] + halves[q + 1] for q in range(depth + 1)]
            others = [weight[0, q, 1 - r] for q in range(depth)]
            for q in range(depth):
                here, up, down = halves[q + 1], downs[q], downs[q + 1]
                inner, outer = here + others[q], here + weight[4, q, r]
                weight[1, q, r] = up
                weight[2, q, r] = down
                if r == 0:
                    weight[3, q, 0] = inner
                weight[4, q, r] = jnp.where(last if r else first, 0.0, outer)
                total = (up + down) + (inner + outer)
                inside = jnp.where(fixed[2, q, r] > 0.0, 1.0, 0.0)
                for mode, real, imag in fields:
                    cosine, sine = wave(levels, mode)
                    denom = total + (1.0 - root * cosine) / time_step
                    if imag is None:
                        inverse[real, q, r] = inside / denom
                    else:
                        shift = root * sine / time_step
                        ratio = inside / (denom * denom + shift * shift)
                        inverse[real, q, r] = ratio * denom
                        inverse[imag, q, r] = ratio * -shift
        for level in range(levels):
            above = None
            ds, ss, inners = [], [], []
            for r in range(2):
                ds.append(rows_around(lambda q: diff[level, q, r]))
                ss.append(rows_around(lambda q: height[level, q, r] + fixed[1, q, r]))
            for q in range(depth):
                inners.append((ds[0][q + 1] + ds[1][q + 1]) * (ss[0][q + 1] - ss[1][q + 1]))
            for r in range(2):
                d, s = ds[r], ss[r]
                downs = [(d[q] + d[q + 1]) * (s[q] - s[q + 1]) for q in range(depth + 1)]
                for q in range(depth):
                    outer = (d[q + 1] + sides[r, level, q]) * (s[q + 1] - sides[2 + r, level, q])
                    across_flux = outer - inners[q] if r else outer + inners[q]
                    prior = height[level - 1, q, r] if level > 0 else fixed[0, q, r]
                    change = (
                        (height[level, q, r] - prior) / time_step
                        + 0.5 * ((downs[q + 1] - downs[q]) + across_flux)
                        - balance[level, q, r]
                    )
                    scaled = change if level == 0 else change * root**level
                    source_part = jnp.where(fixed[2, q, r] > 0.0, scaled, 0.0)
                    diff[level, q, r] = source_part

        def put(f, q, parts):
            value[f, q, 0], value[f, q, 1] = parts
            side[f, q, 0], side[f, q, 1] = before(parts[1]), after(parts[0])

        for q in range(depth):
            scaled = [[diff[level, q, r] for level in range(levels)] for r in range(2)]
            for mode, real, imag in fields:
                waves = [wave(levels, mode * level) for level in range(levels)]
                y_real = [combine([(w[0], v) for w, v in zip(waves, scaled[r])]) for r in range(2)]
                i_real = [inverse[real, q, r] for r in range(2)]
                for r in range(2):
                    source[real, q, r] = y_real[r]
                if imag is None:
                    put(real, q, [i_real[r] * y_real[r] for r in range(2)])
                else:
                    y_imag = [combine([(-w[1], v) for w, v in zip(waves, scaled[r])]) for r in range(2)]
                    i_imag = [inverse[imag, q, r] for r in range(2)]
                    for r in range(2):
                        source[imag, q, r] = y_imag[r]
                    put(real, q, [y_real[r] * i_real[r] - y_imag[r] * i_imag[r] for r in range(2)])
                    put(imag, q, [y_real[r] * i_imag[r] + y_imag[r] * i_real[r] for r in range(2)])

        def sweep(index, carry):
            tops = [[value[f, 0, r] for r in range(2)] for f in range(field_count)]
            befores = [[from_above(value[f, depth - 1, r]) for r in range(2)] for f in range(field_count)]
            heres = tops
            for q in range(depth):
                inner = weight[3, q, 0]
                numer, nexts = [], []
                for f in range(field_count):
                    if q + 1 < depth:
                        nexts.append([value[f, q + 1, r] for r in range(2)])
                    else:
                        nexts.append([from_below(tops[f][r]) for r in range(2)])
                    numer.append([
                        source[f, q, r]
                        + ((weight[1, q, r] * befores[f][r] + weight[2, q, r] * nexts[f][r])
                        + (inner * heres[f][1 - r] + weight[4, q, r] * side[f, q, r]))
                        for r in range(2)
                    ])
                for mode, real, imag in fields:
                    i_real = [inverse[real, q, r] for r in range(2)]
                    if imag is None:
                        put(real, q, [i_real[r] * numer[real][r] for r in range(2)])
                    else:
                        i_imag = [inverse[imag, q, r] for r in range(2)]
                        put(real, q, [numer[real][r] * i_real[r] - numer[imag][r] * i_imag[r] for r in range(2)])
                        put(imag, q, [numer[real][r] * i_imag[r] + numer[imag][r] * i_real[r] for r in range(2)])
                befores, heres = heres, nexts
            return carry

        lax.fori_loop(0, SWEEPS - 1, sweep, 0, unroll=levels <= 8)
        for q in range(depth):
            for r in range(2):
                values = [value[f, q, r] for f in range(field_count)]
                for level in range(levels):
                    scale = 1.0 / (levels * root**level)
                    terms = []
                    for mode, real, imag in fields:
                        cosine, sine = wave(levels, mode * level)
                        if imag is None:
                            terms.append((-scale * cosine, values[real]))
                        else:
                            terms.append((-2.0 * scale * cosine, values[real]))
                            terms.append((2.0 * scale * sine, values[imag]))
                    height[level, q, r] = height[level, q, r] + combine(terms)
        return carry

    lax.fori_loop(0, NEWTON, newton, 0)
    for level in range(levels):
        for q in range(depth):
            even, odd = height[level, q, 0], height[level, q, 1]
            rows = pl.ds(q, SUB, stride=depth)
            plain[level, 0, rows, :] = pick(jnp.where(low, even, half_turn(odd)), mixing)
            plain[level, 1, rows, :] = pick(jnp.where(low, half_turn(even), odd), mixing)
    return plain


def newton_kernel(levels, *refs):
    strips, fixed, take, halo = refs[:levels], *refs[levels : levels + 3]
    outs = refs[levels + 3 : 2 * levels + 3]
    window, spaces = refs[2 * levels + 3], refs[2 * levels + 4 :]
    strip, keep = fixed.shape[1], take.shape[1]
    me, part = lax.axis_index("tm"), lax.axis_index("sy")
    depth = (HALO + keep) // SUB
    window[:, :, :HALO] = halo[...]
    window[:, 1, HALO:] = take[...]
    lay(levels, window.at[:, 0], slice(HALO, HALO + keep), strips, fixed, pl.ds(aligned(part * (strip - keep)), keep))
    plain = newton_steps(levels, lambda field, half, q: window[field, half, pl.ds(q, SUB, stride=depth), :], spaces)
    first = aligned(HALO + part * (keep - strip // 2))
    for shift in range(levels):
        target = lax.rem(me + shift, levels)
        outs[shift][...] = plain[target, :, pl.ds(first, strip // 2)]


def newton_wide_kernel(levels, strip, *refs):
    blocks, outs, spaces = refs[:2], refs[2 : 2 + levels], refs[2 + levels :]
    me = lax.axis_index("tm")
    depth = blocks[0].shape[1] // SUB
    plain = newton_steps(levels, lambda field, half, q: blocks[half][field, pl.ds(q, SUB, stride=depth), :], spaces)
    for shift in range(levels):
        target = lax.rem(me + shift, levels)
        outs[shift][...] = plain[target, 0, HALO : HALO + strip]


def trade_kernel(*refs):
    out = refs[-1]
    for index, ref in enumerate(refs[:-1]):
        out[index] = ref[1]


def place_kernel(levels, strip, *refs):
    pieces, others, out = refs[:levels], refs[levels:-1], refs[-1]
    part = lax.axis_index("sy")
    for shift in range(levels):
        first = strip_of(levels, level_of(levels, shift)) * strip
        if others:
            half = strip // 2
            out[0, pl.ds(aligned(first + part * half), half)] = pieces[shift][0]
            out[0, pl.ds(aligned(first + (1 - part) * half), half)] = others[0][shift]
        else:
            out[0, pl.ds(aligned(first), strip)] = pieces[shift][...]


def call(kernel, name, outs, *operands, scratch=(), spec=vmem):
    return pl.pallas_call(
        kernel,
        out_shape=outs,
        in_specs=[spec] * len(operands),
        out_specs=[vmem] * len(outs) if isinstance(outs, list) else vmem,
        scratch_shapes=list(scratch),
        compiler_params=params,
        name=name,
    )(*operands)


def body(sizes, thickness_guess, thickness_start, bed, rate_factor, mass_balance, cell_flags):
    levels, tiles, parts = sizes
    assert parts == 2
    rows, cols = thickness_start.shape
    strip = rows // levels
    count = 2 * levels + 3
    keep = strip // 2 + HALO

    def swap(value):
        return lax.ppermute(value, "sy", [(0, 1), (1, 0)])

    def around(value, shift):
        return lax.ppermute(value, "tm", [(i, (i + shift) % levels) for i in range(levels)])

    snake = [
        (tm if tile % 2 == 0 else levels - 1 - tm, tile) for tile in range(tiles) for tm in range(levels)
    ]

    def device(place, part):
        tm, tile = snake[place]
        return (tm * tiles + tile) * parts + part

    def along(value, moves):
        pairs = []
        for place in range(len(snake)):
            for part, other, hops in moves:
                if 0 <= place + hops < len(snake):
                    pairs.append((device(place, part), device(place + hops, other)))
        return lax.ppermute(value, ("tm", "sx", "sy"), pairs)

    packed = call(
        functools.partial(pack_kernel, levels, strip),
        "pack",
        [struct(2, strip, cols)] * levels + [struct(3, strip, cols)],
        thickness_guess, mass_balance, thickness_start, bed, rate_factor, cell_flags,
        scratch=(
            pltpu.VMEM((strip, cols), jnp.float32),
            pltpu.VMEM((strip, cols), jnp.int32),
            pltpu.SemaphoreType.DMA((2 * levels + 4,)),
        ),
        spec=hbm,
    )
    strips, fixed = packed[:levels], packed[levels]
    strips = [strips[0]] + [around(strips[shift], shift) for shift in range(1, levels)]

    if strip % (2 * SUB) == 0 and keep <= strip:
        give = call(functools.partial(give_kernel, levels, keep), "give", struct(count, keep, cols), *strips, fixed)
        take = swap(give)
        edge = call(functools.partial(edge_kernel, levels), "edge", struct(count, 2, HALO, cols), *strips, fixed, take)
        halo = along(edge, [(1, 0, 1), (0, 1, -1)])
        high = HALO + keep
        pieces = call(
            functools.partial(newton_kernel, levels),
            "newton",
            [struct(2, strip // 2, cols)] * levels,
            *strips, fixed, take, halo,
            scratch=[pltpu.VMEM((count, 2, high, cols), jnp.float32)]
            + scratches(levels, high // SUB, cols, high),
        )
        pieces = [pieces[0]] + [around(pieces[shift], shift) for shift in range(1, levels)]
        others = [swap(call(trade_kernel, "trade", struct(levels, strip // 2, cols), *pieces))]
    else:
        counts = [min(strip, HALO - done) for done in range(0, HALO, strip)]
        rims = call(
            functools.partial(rim_kernel, levels, counts),
            "rim",
            [struct(count, n, cols) for n in counts] * 2,
            *strips, fixed,
        )
        aboves = [along(rims[len(counts) + i], [(0, 0, i + 1), (1, 1, i + 1)]) for i in range(len(counts))]
        belows = [along(rims[i], [(0, 0, -i - 1), (1, 1, -i - 1)]) for i in range(len(counts))]
        high = strip + 2 * HALO
        mine = call(
            functools.partial(join_kernel, levels, counts),
            "join",
            struct(count, high, cols),
            *strips, fixed, *aboves, *belows,
        )
        pieces = call(
            functools.partial(newton_wide_kernel, levels, strip),
            "newton",
            [struct(strip, cols)] * levels,
            mine, swap(mine),
            scratch=scratches(levels, high // SUB, cols, high),
        )
        pieces = [pieces[0]] + [around(pieces[shift], shift) for shift in range(1, levels)]
        others = []
    return call(functools.partial(place_kernel, levels, strip), "place", struct(1, rows, cols), *pieces, *others)


def solution(mesh):
    sizes = tuple(mesh.shape[axis] for axis in ("tm", "sx", "sy"))
    in_specs = (
        P("tm", "sx", "sy"),
        P("sx", "sy"),
        P("sx", "sy"),
        P("sx", "sy"),
        P("tm", "sx", "sy"),
        P("sx", "sy"),
    )
    out_specs = P("tm", "sx", "sy")
    return jax.shard_map(
        functools.partial(body, sizes), mesh=mesh, in_specs=in_specs, out_specs=out_specs, check_vma=False
    )
```

```python
import functools
import math

import jax
import jax.numpy as jnp
from jax import lax
from jax.experimental import pallas as pl
from jax.experimental.pallas import tpu as pltpu
from jax.sharding import PartitionSpec as P

NEWTON = 2
SWEEPS = 8
HALO = NEWTON * SWEEPS
SUB = 8

circulant_weight = 0.25
time_step = 1.0


vmem = pl.BlockSpec(memory_space=pltpu.VMEM)
hbm = pl.BlockSpec(memory_space=pltpu.HBM)
params = pltpu.CompilerParams(vmem_limit_bytes=16 * 1024 * 1024)

fetching = pltpu.CompilerParams(vmem_limit_bytes=56125000)


def struct(*shape):
    return jax.ShapeDtypeStruct(shape, jnp.float32)


def aligned(index):
    return pl.multiple_of(index, SUB)


def strip_of(levels, tm):
    return jnp.where(lax.rem(lax.axis_index("sx"), 2) == 0, tm, levels - 1 - tm)


def level_of(levels, shift):
    return lax.rem(lax.axis_index("tm") + levels - shift, levels)


def pick(array, index):
    return jnp.take_along_axis(array, index, axis=1, mode="promise_in_bounds")


def pack_kernel(levels, strip, *refs):
    guess, balance, start, bed, rate, flags = refs[:6]
    strips = refs[6 : 6 + levels]
    fixed, ice, kind, sems = refs[6 + levels :]
    me = lax.axis_index("tm")

    def rows_of(tm):
        return pl.ds(aligned(strip_of(levels, tm) * strip), strip)

    copies = []
    for shift in range(levels):
        here = rows_of(lax.rem(me + shift, levels))
        copies += [(guess.at[0, here], strips[shift].at[0]), (balance.at[0, here], strips[shift].at[1])]
    here = rows_of(me)
    copies += [
        (start.at[here], fixed.at[0]),
        (bed.at[here], fixed.at[1]),
        (rate.at[here], ice),
        (flags.at[here], kind),
    ]
    copies = [pltpu.make_async_copy(a, b, sems.at[i]) for i, (a, b) in enumerate(copies)]
    for copy in copies:
        copy.start()
    for copy in copies:
        copy.wait()
    boost = jnp.where(kind[...] == 2, 2.0, 1.0)
    fixed[2] = jnp.where(kind[...] != 0, boost * ice[...], 0.0)
    cols = fixed.shape[2]
    lane = lax.broadcasted_iota(jnp.int32, (SUB, cols), 1)
    parting = jnp.where(lane < cols // 2, 2 * lane, 2 * lane - (cols - 1))
    for ref in (*strips, fixed):
        for index in range(ref.shape[0]):
            for row in range(0, strip, SUB):
                ref[index, row : row + SUB] = pick(ref[index, row : row + SUB], parting)


def lay(levels, out, rows, strips, fixed, source):
    for shift in range(levels):
        level = level_of(levels, shift)
        out[level, rows] = strips[shift][0, source]
        out[levels + level, rows] = strips[shift][1, source]
    out[2 * levels :, rows] = fixed[:, source]


def give_kernel(levels, keep, *refs):
    strips, fixed, out = refs[:levels], refs[levels], refs[-1]
    strip = fixed.shape[1]
    first = aligned((1 - lax.axis_index("sy")) * (strip - keep))
    lay(levels, out, slice(0, keep), strips, fixed, pl.ds(first, keep))


def edge_kernel(levels, *refs):
    strips, fixed, take, out = refs[:levels], refs[levels], refs[levels + 1], refs[-1]
    strip, keep = fixed.shape[1], take.shape[1]
    part = lax.axis_index("sy")
    out[:, 0] = take[:, pl.ds(aligned(part * (keep - HALO)), HALO)]
    source = pl.ds(aligned(part * (strip - HALO)), HALO)
    for shift in range(levels):
        level = level_of(levels, shift)
        out[level, 1] = strips[shift][0, source]
        out[levels + level, 1] = strips[shift][1, source]
    out[2 * levels :, 1] = fixed[:, source]


def rim_kernel(levels, counts, *refs):
    strips = refs[:levels]
    fixed = refs[levels]
    lows, highs = refs[levels + 1 : levels + 1 + len(counts)], refs[levels + 1 + len(counts) :]
    strip = fixed.shape[1]
    for count, low, high in zip(counts, lows, highs):
        lay(levels, low, slice(0, count), strips, fixed, slice(0, count))
        lay(levels, high, slice(0, count), strips, fixed, slice(strip - count, strip))


def join_kernel(levels, counts, *refs):
    strips = refs[:levels]
    fixed = refs[levels]
    aboves, belows = refs[levels + 1 : levels + 1 + len(counts)], refs[levels + 1 + len(counts) : -1]
    out = refs[-1]
    strip = fixed.shape[1]
    lay(levels, out, slice(HALO, HALO + strip), strips, fixed, slice(0, strip))
    done = 0
    for count, above, below in zip(counts, aboves, belows):
        out[:, HALO - done - count : HALO - done] = above[...]
        out[:, HALO + strip + done : HALO + strip + done + count] = below[...]
        done += count


def mode_fields(levels):
    fields, count = [], 0
    for mode in range(levels // 2 + 1):
        if 2 * mode % levels == 0:
            fields.append((mode, count, None))
            count += 1
        else:
            fields.append((mode, count, count + 1))
            count += 2
    return fields, count


def wave(levels, product):
    product %= levels
    quarter = 4 * product
    if quarter % levels == 0:
        return ((1.0, 0.0), (0.0, 1.0), (-1.0, 0.0), (0.0, -1.0))[quarter // levels]
    angle = 2.0 * math.pi * product / levels
    return math.cos(angle), math.sin(angle)


def combine(terms):
    total = None
    for coeff, value in terms:
        if coeff == 0.0:
            continue
        if total is None:
            total = value if coeff == 1.0 else coeff * value
        elif coeff == 1.0:
            total = total + value
        elif coeff == -1.0:
            total = total - value
        else:
            total = total + coeff * value
    return total


def scratches(levels, depth, cols, high):
    _, field_count = mode_fields(levels)
    shapes = [(count, depth, 2, SUB, cols) for count in (levels, levels, 3, levels, 5, *(field_count,) * 4)]
    shapes.append((4, levels, depth, SUB, cols))
    shapes.append((levels, 2, high, cols))
    return [pltpu.VMEM(shape, jnp.float32) for shape in shapes]


def newton_steps(levels, load, spaces):
    height, balance, fixed, diff, weight, inverse, source, value, side, sides, plain = spaces
    depth, _, _, cols = height.shape[1:]
    across = 2 * cols
    lane = lax.broadcasted_iota(jnp.int32, (SUB, cols), 1)
    low = lane < cols // 2
    column = lax.axis_index("sy") * cols
    first = 2 * lane == lax.rem(across - column, across)
    last = 2 * lane + 1 == across - 1 - column
    fields, field_count = mode_fields(levels)
    root = circulant_weight ** (1.0 / levels)

    def half_turn(array):
        return pltpu.roll(array, cols // 2, axis=1)

    def before(odd):
        return pltpu.roll(odd, 1, axis=1)

    def after(even):
        return pltpu.roll(even, cols - 1, axis=1)

    def from_above(array):
        return pltpu.roll(array, 1, axis=0)

    def from_below(array):
        return pltpu.roll(array, SUB - 1, axis=0)

    def rows_around(read):
        blocks = [read(q) for q in range(depth)]
        return [from_above(blocks[-1])] + blocks + [from_below(blocks[0])]

    places = [(height, level, level) for level in range(levels)]
    places += [(balance, level, levels + level) for level in range(levels)]
    places += [(fixed, index, 2 * levels + index) for index in range(3)]
    for ref, index, field in places:
        for q in range(depth):
            left, right = (load(field, half, q) for half in range(2))
            ref[index, q, 0] = jnp.where(low, left, half_turn(right))
            ref[index, q, 1] = jnp.where(low, half_turn(left), right)

    def newton(step, carry):
        for q in range(depth):
            totals = [None] * 4
            for level in range(levels):
                thick = [height[level, q, r] for r in range(2)]
                d = [fixed[2, q, r] * thick[r] * thick[r] * jnp.abs(thick[r]) for r in range(2)]
                s = [thick[r] + fixed[1, q, r] for r in range(2)]
                for r in range(2):
                    diff[level, q, r] = d[r]
                d_left, d_right = jnp.where(first, 0.0, before(d[1])), jnp.where(last, 0.0, after(d[0]))
                sides[0, level, q] = d_left
                sides[1, level, q] = d_right
                sides[2, level, q] = jnp.where(first, 0.0, before(s[1]))
                sides[3, level, q] = jnp.where(last, 0.0, after(s[0]))
                for i, part in enumerate((d[0], d[1], d_left, d_right)):
                    totals[i] = part if level == 0 else totals[i] + part
            even, odd, left, right = (total * (0.5 / levels) for total in totals)
            weight[0, q, 0], weight[0, q, 1] = even, odd
            weight[4, q, 0], weight[4, q, 1] = left, right
        for r in range(2):
            halves = rows_around(lambda q: weight[0, q, r])
            downs = [halves[q] + halves[q + 1] for q in range(depth + 1)]
            others = [weight[0, q, 1 - r] for q in range(depth)]
            for q in range(depth):
                here, up, down = halves[q + 1], downs[q], downs[q + 1]
                inner, outer = here + others[q], here + weight[4, q, r]
                weight[1, q, r] = up
                weight[2, q, r] = down
                if r == 0:
                    weight[3, q, 0] = inner
                weight[4, q, r] = jnp.where(last if r else first, 0.0, outer)
                total = (up + down) + (inner + outer)
                inside = jnp.where(fixed[2, q, r] > 0.0, 1.0, 0.0)
                for mode, real, imag in fields:
                    cosine, sine = wave(levels, mode)
                    denom = total + (1.0 - root * cosine) / time_step
                    if imag is None:
                        inverse[real, q, r] = inside / denom
                    else:
                        shift = root * sine / time_step
                        ratio = inside / (denom * denom + shift * shift)
                        inverse[real, q, r] = ratio * denom
                        inverse[imag, q, r] = ratio * -shift
        for level in range(levels):
            above = None
            ds, ss, inners = [], [], []
            for r in range(2):
                ds.append(rows_around(lambda q: diff[level, q, r]))
                ss.append(rows_around(lambda q: height[level, q, r] + fixed[1, q, r]))
            for q in range(depth):
                inners.append((ds[0][q + 1] + ds[1][q + 1]) * (ss[0][q + 1] - ss[1][q + 1]))
            for r in range(2):
                d, s = ds[r], ss[r]
                downs = [(d[q] + d[q + 1]) * (s[q] - s[q + 1]) for q in range(depth + 1)]
                for q in range(depth):
                    outer = (d[q + 1] + sides[r, level, q]) * (s[q + 1] - sides[2 + r, level, q])
                    across_flux = outer - inners[q] if r else outer + inners[q]
                    prior = height[level - 1, q, r] if level > 0 else fixed[0, q, r]
                    change = (
                        (height[level, q, r] - prior) / time_step
                        + 0.5 * ((downs[q + 1] - downs[q]) + across_flux)
                        - balance[level, q, r]
                    )
                    scaled = change if level == 0 else change * root**level
                    source_part = jnp.where(fixed[2, q, r] > 0.0, scaled, 0.0)
                    diff[level, q, r] = source_part

        def put(f, q, parts):
            value[f, q, 0], value[f, q, 1] = parts
            side[f, q, 0], side[f, q, 1] = before(parts[1]), after(parts[0])

        for q in range(depth):
            scaled = [[diff[level, q, r] for level in range(levels)] for r in range(2)]
            for mode, real, imag in fields:
                waves = [wave(levels, mode * level) for level in range(levels)]
                y_real = [combine([(w[0], v) for w, v in zip(waves, scaled[r])]) for r in range(2)]
                i_real = [inverse[real, q, r] for r in range(2)]
                for r in range(2):
                    source[real, q, r] = y_real[r]
                if imag is None:
                    put(real, q, [i_real[r] * y_real[r] for r in range(2)])
                else:
                    y_imag = [combine([(-w[1], v) for w, v in zip(waves, scaled[r])]) for r in range(2)]
                    i_imag = [inverse[imag, q, r] for r in range(2)]
                    for r in range(2):
                        source[imag, q, r] = y_imag[r]
                    put(real, q, [y_real[r] * i_real[r] - y_imag[r] * i_imag[r] for r in range(2)])
                    put(imag, q, [y_real[r] * i_imag[r] + y_imag[r] * i_real[r] for r in range(2)])

        def sweep(index, carry):
            tops = [[value[f, 0, r] for r in range(2)] for f in range(field_count)]
            befores = [[from_above(value[f, depth - 1, r]) for r in range(2)] for f in range(field_count)]
            heres = tops
            for q in range(depth):
                inner = weight[3, q, 0]
                numer, nexts = [], []
                for f in range(field_count):
                    if q + 1 < depth:
                        nexts.append([value[f, q + 1, r] for r in range(2)])
                    else:
                        nexts.append([from_below(tops[f][r]) for r in range(2)])
                    numer.append([
                        source[f, q, r]
                        + ((weight[1, q, r] * befores[f][r] + weight[2, q, r] * nexts[f][r])
                        + (inner * heres[f][1 - r] + weight[4, q, r] * side[f, q, r]))
                        for r in range(2)
                    ])
                for mode, real, imag in fields:
                    i_real = [inverse[real, q, r] for r in range(2)]
                    if imag is None:
                        put(real, q, [i_real[r] * numer[real][r] for r in range(2)])
                    else:
                        i_imag = [inverse[imag, q, r] for r in range(2)]
                        put(real, q, [numer[real][r] * i_real[r] - numer[imag][r] * i_imag[r] for r in range(2)])
                        put(imag, q, [numer[real][r] * i_imag[r] + numer[imag][r] * i_real[r] for r in range(2)])
                befores, heres = heres, nexts
            return carry

        lax.fori_loop(0, SWEEPS - 1, sweep, 0, unroll=levels <= 8)
        for q in range(depth):
            for r in range(2):
                values = [value[f, q, r] for f in range(field_count)]
                for level in range(levels):
                    scale = 1.0 / (levels * root**level)
                    terms = []
                    for mode, real, imag in fields:
                        cosine, sine = wave(levels, mode * level)
                        if imag is None:
                            terms.append((-scale * cosine, values[real]))
                        else:
                            terms.append((-2.0 * scale * cosine, values[real]))
                            terms.append((2.0 * scale * sine, values[imag]))
                    height[level, q, r] = height[level, q, r] + combine(terms)
        return carry

    lax.fori_loop(0, NEWTON, newton, 0)
    for level in range(levels):
        for q in range(depth):
            even, odd = height[level, q, 0], height[level, q, 1]
            rows = pl.ds(q, SUB, stride=depth)
            plain[level, 0, rows, :] = jnp.where(low, even, half_turn(odd))
            plain[level, 1, rows, :] = jnp.where(low, half_turn(even), odd)
    return plain


def newton_kernel(levels, *refs):
    strips, fixed, take, halo = refs[:levels], *refs[levels : levels + 3]
    outs = refs[levels + 3 : 2 * levels + 3]
    window, spaces = refs[2 * levels + 3], refs[2 * levels + 4 :]
    strip, keep = fixed.shape[1], take.shape[1]
    me, part = lax.axis_index("tm"), lax.axis_index("sy")
    depth = (HALO + keep) // SUB
    window[:, :, :HALO] = halo[...]
    window[:, 1, HALO:] = take[...]
    lay(levels, window.at[:, 0], slice(HALO, HALO + keep), strips, fixed, pl.ds(aligned(part * (strip - keep)), keep))
    plain = newton_steps(levels, lambda field, half, q: window[field, half, pl.ds(q, SUB, stride=depth), :], spaces)
    first = aligned(HALO + part * (keep - strip // 2))
    for shift in range(levels):
        target = lax.rem(me + shift, levels)
        outs[shift][...] = plain[target, :, pl.ds(first, strip // 2)]


def newton_wide_kernel(levels, strip, *refs):
    blocks, outs, spaces = refs[:2], refs[2 : 2 + levels], refs[2 + levels :]
    me = lax.axis_index("tm")
    depth = blocks[0].shape[1] // SUB
    plain = newton_steps(levels, lambda field, half, q: blocks[half][field, pl.ds(q, SUB, stride=depth), :], spaces)
    for shift in range(levels):
        target = lax.rem(me + shift, levels)
        outs[shift][...] = plain[target, 0, HALO : HALO + strip]


def trade_kernel(*refs):
    out = refs[-1]
    for index, ref in enumerate(refs[:-1]):
        out[index] = ref[1]


def place_kernel(levels, strip, *refs):
    pieces, others, out = refs[:levels], refs[levels:-1], refs[-1]
    part = lax.axis_index("sy")
    cols = out.shape[2]
    lane = lax.broadcasted_iota(jnp.int32, (SUB, cols), 1)
    mixing = lane // 2 + lane % 2 * (cols // 2)

    def put(first, piece):
        for row in range(0, piece.shape[0], SUB):
            out[0, pl.ds(aligned(first + row), SUB)] = pick(piece[row : row + SUB], mixing)

    for shift in range(levels):
        first = strip_of(levels, level_of(levels, shift)) * strip
        if others:
            half = strip // 2
            put(first + part * half, pieces[shift].at[0])
            put(first + (1 - part) * half, others[0].at[shift])
        else:
            put(first, pieces[shift])


def call(kernel, name, outs, *operands, scratch=(), spec=vmem, params=params):
    return pl.pallas_call(
        kernel,
        out_shape=outs,
        in_specs=[spec] * len(operands),
        out_specs=[vmem] * len(outs) if isinstance(outs, list) else vmem,
        scratch_shapes=list(scratch),
        compiler_params=params,
        name=name,
    )(*operands)


def body(sizes, thickness_guess, thickness_start, bed, rate_factor, mass_balance, cell_flags):
    levels, tiles, parts = sizes
    assert parts == 2
    rows, cols = thickness_start.shape
    strip = rows // levels
    count = 2 * levels + 3
    keep = strip // 2 + HALO

    def swap(value):
        return lax.ppermute(value, "sy", [(0, 1), (1, 0)])

    def around(value, shift):
        return lax.ppermute(value, "tm", [(i, (i + shift) % levels) for i in range(levels)])

    snake = [
        (tm if tile % 2 == 0 else levels - 1 - tm, tile) for tile in range(tiles) for tm in range(levels)
    ]

    def device(place, part):
        tm, tile = snake[place]
        return (tm * tiles + tile) * parts + part

    def along(value, moves):
        pairs = []
        for place in range(len(snake)):
            for part, other, hops in moves:
                if 0 <= place + hops < len(snake):
                    pairs.append((device(place, part), device(place + hops, other)))
        return lax.ppermute(value, ("tm", "sx", "sy"), pairs)

    packed = call(
        functools.partial(pack_kernel, levels, strip),
        "pack",
        [struct(2, strip, cols)] * levels + [struct(3, strip, cols)],
        thickness_guess, mass_balance, thickness_start, bed, rate_factor, cell_flags,
        scratch=(
            pltpu.VMEM((strip, cols), jnp.float32),
            pltpu.VMEM((strip, cols), jnp.int32),
            pltpu.SemaphoreType.DMA((2 * levels + 4,)),
        ),
        spec=hbm,
        params=fetching,
    )
    strips, fixed = packed[:levels], packed[levels]
    strips = [strips[0]] + [around(strips[shift], shift) for shift in range(1, levels)]

    if strip % (2 * SUB) == 0 and keep <= strip:
        give = call(functools.partial(give_kernel, levels, keep), "give", struct(count, keep, cols), *strips, fixed)
        take = swap(give)
        edge = call(functools.partial(edge_kernel, levels), "edge", struct(count, 2, HALO, cols), *strips, fixed, take)
        halo = along(edge, [(1, 0, 1), (0, 1, -1)])
        high = HALO + keep
        pieces = call(
            functools.partial(newton_kernel, levels),
            "newton",
            [struct(2, strip // 2, cols)] * levels,
            *strips, fixed, take, halo,
            scratch=[pltpu.VMEM((count, 2, high, cols), jnp.float32)]
            + scratches(levels, high // SUB, cols, high),
        )
        pieces = [pieces[0]] + [around(pieces[shift], shift) for shift in range(1, levels)]
        others = [swap(call(trade_kernel, "trade", struct(levels, strip // 2, cols), *pieces))]
    else:
        counts = [min(strip, HALO - done) for done in range(0, HALO, strip)]
        rims = call(
            functools.partial(rim_kernel, levels, counts),
            "rim",
            [struct(count, n, cols) for n in counts] * 2,
            *strips, fixed,
        )
        aboves = [along(rims[len(counts) + i], [(0, 0, i + 1), (1, 1, i + 1)]) for i in range(len(counts))]
        belows = [along(rims[i], [(0, 0, -i - 1), (1, 1, -i - 1)]) for i in range(len(counts))]
        high = strip + 2 * HALO
        mine = call(
            functools.partial(join_kernel, levels, counts),
            "join",
            struct(count, high, cols),
            *strips, fixed, *aboves, *belows,
        )
        pieces = call(
            functools.partial(newton_wide_kernel, levels, strip),
            "newton",
            [struct(strip, cols)] * levels,
            mine, swap(mine),
            scratch=scratches(levels, high // SUB, cols, high),
        )
        pieces = [pieces[0]] + [around(pieces[shift], shift) for shift in range(1, levels)]
        others = []
    return call(functools.partial(place_kernel, levels, strip), "place", struct(1, rows, cols), *pieces, *others)


def solution(mesh):
    sizes = tuple(mesh.shape[axis] for axis in ("tm", "sx", "sy"))
    in_specs = (
        P("tm", "sx", "sy"),
        P("sx", "sy"),
        P("sx", "sy"),
        P("sx", "sy"),
        P("tm", "sx", "sy"),
        P("sx", "sy"),
    )
    out_specs = P("tm", "sx", "sy")
    return jax.shard_map(
        functools.partial(body, sizes), mesh=mesh, in_specs=in_specs, out_specs=out_specs, check_vma=False
    )
```

```python
import functools
import math

import jax
import jax.numpy as jnp
from jax import lax
from jax.experimental import pallas as pl
from jax.experimental.pallas import tpu as pltpu
from jax.sharding import PartitionSpec as P


NEWTON = 2
SWEEPS = 8
HALO = NEWTON * SWEEPS
SUB = 8

circulant_weight = 0.25
time_step = 1.0


vmem = pl.BlockSpec(memory_space=pltpu.VMEM)
hbm = pl.BlockSpec(memory_space=pltpu.HBM)
params = pltpu.CompilerParams(vmem_limit_bytes=16 * 1024 * 1024)

fetching = pltpu.CompilerParams(vmem_limit_bytes=56125000)


def struct(*shape):
    return jax.ShapeDtypeStruct(shape, jnp.float32)


def aligned(index):
    return pl.multiple_of(index, SUB)


def strip_of(levels, tm):
    return jnp.where(lax.rem(lax.axis_index("sx"), 2) == 0, tm, levels - 1 - tm)


def level_of(levels, shift):
    return lax.rem(lax.axis_index("tm") + levels - shift, levels)


def pick(array, index):
    return jnp.take_along_axis(array, index, axis=1, mode="promise_in_bounds")


def pack_kernel(levels, strip, *refs):
    guess, balance, start, bed, rate, flags = refs[:6]
    strips = refs[6 : 6 + levels]
    fixed, ice, kind, sems = refs[6 + levels :]
    me = lax.axis_index("tm")

    def rows_of(tm):
        return pl.ds(aligned(strip_of(levels, tm) * strip), strip)

    copies = []
    for shift in range(levels):
        here = rows_of(lax.rem(me + shift, levels))
        copies += [(guess.at[0, here], strips[shift].at[0]), (balance.at[0, here], strips[shift].at[1])]
    here = rows_of(me)
    copies += [
        (start.at[here], fixed.at[0]),
        (bed.at[here], fixed.at[1]),
        (rate.at[here], ice),
        (flags.at[here], kind),
    ]
    copies = [pltpu.make_async_copy(a, b, sems.at[i]) for i, (a, b) in enumerate(copies)]
    for copy in copies:
        copy.start()
    for copy in copies:
        copy.wait()
    boost = jnp.where(kind[...] == 2, 2.0, 1.0)
    fixed[2] = jnp.where(kind[...] != 0, boost * ice[...], 0.0)
    cols = fixed.shape[2]
    lane = lax.broadcasted_iota(jnp.int32, (SUB, cols), 1)
    parting = jnp.where(lane < cols // 2, 2 * lane, 2 * lane - (cols - 1))
    for ref in (*strips, fixed):
        for index in range(ref.shape[0]):
            for row in range(0, strip, SUB):
                ref[index, row : row + SUB] = pick(ref[index, row : row + SUB], parting)


def lay(levels, out, rows, strips, fixed, source):
    for shift in range(levels):
        level = level_of(levels, shift)
        out[level, rows] = strips[shift][0, source]
        out[levels + level, rows] = strips[shift][1, source]
    out[2 * levels :, rows] = fixed[:, source]


def give_kernel(*refs):
    out, place = refs[-1], 0
    keep = out.shape[1]
    for ref in refs[:-1]:
        count, strip, _ = ref.shape
        first = aligned((1 - lax.axis_index("sy")) * (strip - keep))
        out[place : place + count] = ref[:, pl.ds(first, keep)]
        place += count


def lay_taken(levels, out, index, early, late, source):
    for shift in range(levels):
        level = level_of(levels, shift)
        ref, place = (early, 2 * shift) if shift < levels - 1 else (late, 0)
        out[(level, *index)] = ref[place, source]
        out[(levels + level, *index)] = ref[place + 1, source]
    out[(slice(2 * levels, None), *index)] = early[2 * levels - 2 :, source]


def edge_kernel(levels, *refs):
    strips, fixed, early, late, out = refs[:levels], *refs[levels:]
    strip, keep = fixed.shape[1], late.shape[1]
    part = lax.axis_index("sy")
    lay_taken(levels, out, (0,), early, late, pl.ds(aligned(part * (keep - HALO)), HALO))
    source = pl.ds(aligned(part * (strip - HALO)), HALO)
    lay(levels, out.at[:, 1], slice(0, HALO), strips, fixed, source)


def rim_kernel(levels, counts, *refs):
    strips = refs[:levels]
    fixed = refs[levels]
    lows, highs = refs[levels + 1 : levels + 1 + len(counts)], refs[levels + 1 + len(counts) :]
    strip = fixed.shape[1]
    for count, low, high in zip(counts, lows, highs):
        lay(levels, low, slice(0, count), strips, fixed, slice(0, count))
        lay(levels, high, slice(0, count), strips, fixed, slice(strip - count, strip))


def join_kernel(levels, counts, *refs):
    strips = refs[:levels]
    fixed = refs[levels]
    aboves, belows = refs[levels + 1 : levels + 1 + len(counts)], refs[levels + 1 + len(counts) : -1]
    out = refs[-1]
    strip = fixed.shape[1]
    lay(levels, out, slice(HALO, HALO + strip), strips, fixed, slice(0, strip))
    done = 0
    for count, above, below in zip(counts, aboves, belows):
        out[:, HALO - done - count : HALO - done] = above[...]
        out[:, HALO + strip + done : HALO + strip + done + count] = below[...]
        done += count


def mode_fields(levels):
    fields, count = [], 0
    for mode in range(levels // 2 + 1):
        if 2 * mode % levels == 0:
            fields.append((mode, count, None))
            count += 1
        else:
            fields.append((mode, count, count + 1))
            count += 2
    return fields, count


def wave(levels, product):
    product %= levels
    quarter = 4 * product
    if quarter % levels == 0:
        return ((1.0, 0.0), (0.0, 1.0), (-1.0, 0.0), (0.0, -1.0))[quarter // levels]
    angle = 2.0 * math.pi * product / levels
    return math.cos(angle), math.sin(angle)


def combine(terms):
    total = None
    for coeff, value in terms:
        if coeff == 0.0:
            continue
        if total is None:
            total = value if coeff == 1.0 else coeff * value
        elif coeff == 1.0:
            total = total + value
        elif coeff == -1.0:
            total = total - value
        else:
            total = total + coeff * value
    return total


def scratches(levels, depth, cols, high):
    _, field_count = mode_fields(levels)
    shapes = [(count, depth, 2, SUB, cols) for count in (levels, levels, 3, levels, 5, *(field_count,) * 4)]
    shapes.append((4, levels, depth, SUB, cols))
    shapes.append((levels, 2, high, cols))
    return [pltpu.VMEM(shape, jnp.float32) for shape in shapes]


def newton_steps(levels, load, spaces):
    height, balance, fixed, diff, weight, inverse, source, value, side, sides, plain = spaces
    depth, _, _, cols = height.shape[1:]
    across = 2 * cols
    lane = lax.broadcasted_iota(jnp.int32, (SUB, cols), 1)
    low = lane < cols // 2
    column = lax.axis_index("sy") * cols
    first = 2 * lane == lax.rem(across - column, across)
    last = 2 * lane + 1 == across - 1 - column
    fields, field_count = mode_fields(levels)
    root = circulant_weight ** (1.0 / levels)

    def half_turn(array):
        return pltpu.roll(array, cols // 2, axis=1)

    def before(odd):
        return pltpu.roll(odd, 1, axis=1)

    def after(even):
        return pltpu.roll(even, cols - 1, axis=1)

    def from_above(array):
        return pltpu.roll(array, 1, axis=0)

    def from_below(array):
        return pltpu.roll(array, SUB - 1, axis=0)

    def rows_around(read):
        blocks = [read(q) for q in range(depth)]
        return [from_above(blocks[-1])] + blocks + [from_below(blocks[0])]

    places = [(height, level, level) for level in range(levels)]
    places += [(balance, level, levels + level) for level in range(levels)]
    places += [(fixed, index, 2 * levels + index) for index in range(3)]
    for ref, index, field in places:
        for q in range(depth):
            left, right = (load(field, half, q) for half in range(2))
            ref[index, q, 0] = jnp.where(low, left, half_turn(right))
            ref[index, q, 1] = jnp.where(low, half_turn(left), right)

    def newton(step, carry):
        for q in range(depth):
            totals = [None] * 4
            for level in range(levels):
                thick = [height[level, q, r] for r in range(2)]
                d = [fixed[2, q, r] * thick[r] * thick[r] * jnp.abs(thick[r]) for r in range(2)]
                s = [thick[r] + fixed[1, q, r] for r in range(2)]
                for r in range(2):
                    diff[level, q, r] = d[r]
                d_left, d_right = jnp.where(first, 0.0, before(d[1])), jnp.where(last, 0.0, after(d[0]))
                sides[0, level, q] = d_left
                sides[1, level, q] = d_right
                sides[2, level, q] = jnp.where(first, 0.0, before(s[1]))
                sides[3, level, q] = jnp.where(last, 0.0, after(s[0]))
                for i, part in enumerate((d[0], d[1], d_left, d_right)):
                    totals[i] = part if level == 0 else totals[i] + part
            even, odd, left, right = (total * (0.5 / levels) for total in totals)
            weight[0, q, 0], weight[0, q, 1] = even, odd
            weight[4, q, 0], weight[4, q, 1] = left, right
        for r in range(2):
            halves = rows_around(lambda q: weight[0, q, r])
            downs = [halves[q] + halves[q + 1] for q in range(depth + 1)]
            others = [weight[0, q, 1 - r] for q in range(depth)]
            for q in range(depth):
                here, up, down = halves[q + 1], downs[q], downs[q + 1]
                inner, outer = here + others[q], here + weight[4, q, r]
                weight[1, q, r] = up
                weight[2, q, r] = down
                if r == 0:
                    weight[3, q, 0] = inner
                weight[4, q, r] = jnp.where(last if r else first, 0.0, outer)
                total = (up + down) + (inner + outer)
                inside = jnp.where(fixed[2, q, r] > 0.0, 1.0, 0.0)
                for mode, real, imag in fields:
                    cosine, sine = wave(levels, mode)
                    denom = total + (1.0 - root * cosine) / time_step
                    if imag is None:
                        inverse[real, q, r] = inside / denom
                    else:
                        shift = root * sine / time_step
                        ratio = inside / (denom * denom + shift * shift)
                        inverse[real, q, r] = ratio * denom
                        inverse[imag, q, r] = ratio * -shift
        for level in range(levels):
            ds, ss, inners = [], [], []
            for r in range(2):
                ds.append(rows_around(lambda q: diff[level, q, r]))
                ss.append(rows_around(lambda q: height[level, q, r] + fixed[1, q, r]))
            for q in range(depth):
                inners.append((ds[0][q + 1] + ds[1][q + 1]) * (ss[0][q + 1] - ss[1][q + 1]))
            for r in range(2):
                d, s = ds[r], ss[r]
                downs = [(d[q] + d[q + 1]) * (s[q] - s[q + 1]) for q in range(depth + 1)]
                for q in range(depth):
                    outer = (d[q + 1] + sides[r, level, q]) * (s[q + 1] - sides[2 + r, level, q])
                    across_flux = outer - inners[q] if r else outer + inners[q]
                    prior = height[level - 1, q, r] if level > 0 else fixed[0, q, r]
                    change = (
                        (height[level, q, r] - prior) / time_step
                        + 0.5 * ((downs[q + 1] - downs[q]) + across_flux)
                        - balance[level, q, r]
                    )
                    scaled = change if level == 0 else change * root**level
                    source_part = jnp.where(fixed[2, q, r] > 0.0, scaled, 0.0)
                    diff[level, q, r] = source_part

        def put(f, q, parts):
            value[f, q, 0], value[f, q, 1] = parts
            side[f, q, 0], side[f, q, 1] = before(parts[1]), after(parts[0])

        for q in range(depth):
            scaled = [[diff[level, q, r] for level in range(levels)] for r in range(2)]
            for mode, real, imag in fields:
                waves = [wave(levels, mode * level) for level in range(levels)]
                y_real = [combine([(w[0], v) for w, v in zip(waves, scaled[r])]) for r in range(2)]
                i_real = [inverse[real, q, r] for r in range(2)]
                for r in range(2):
                    source[real, q, r] = y_real[r]
                if imag is None:
                    put(real, q, [i_real[r] * y_real[r] for r in range(2)])
                else:
                    y_imag = [combine([(-w[1], v) for w, v in zip(waves, scaled[r])]) for r in range(2)]
                    i_imag = [inverse[imag, q, r] for r in range(2)]
                    for r in range(2):
                        source[imag, q, r] = y_imag[r]
                    put(real, q, [y_real[r] * i_real[r] - y_imag[r] * i_imag[r] for r in range(2)])
                    put(imag, q, [y_real[r] * i_imag[r] + y_imag[r] * i_real[r] for r in range(2)])

        def sweep(index, carry):
            tops = [[value[f, 0, r] for r in range(2)] for f in range(field_count)]
            befores = [[from_above(value[f, depth - 1, r]) for r in range(2)] for f in range(field_count)]
            heres = tops
            for q in range(depth):
                inner = weight[3, q, 0]
                numer, nexts = [], []
                for f in range(field_count):
                    if q + 1 < depth:
                        nexts.append([value[f, q + 1, r] for r in range(2)])
                    else:
                        nexts.append([from_below(tops[f][r]) for r in range(2)])
                    numer.append([
                        source[f, q, r]
                        + ((weight[1, q, r] * befores[f][r] + weight[2, q, r] * nexts[f][r])
                        + (inner * heres[f][1 - r] + weight[4, q, r] * side[f, q, r]))
                        for r in range(2)
                    ])
                for mode, real, imag in fields:
                    i_real = [inverse[real, q, r] for r in range(2)]
                    if imag is None:
                        put(real, q, [i_real[r] * numer[real][r] for r in range(2)])
                    else:
                        i_imag = [inverse[imag, q, r] for r in range(2)]
                        put(real, q, [numer[real][r] * i_real[r] - numer[imag][r] * i_imag[r] for r in range(2)])
                        put(imag, q, [numer[real][r] * i_imag[r] + numer[imag][r] * i_real[r] for r in range(2)])
                befores, heres = heres, nexts
            return carry

        lax.fori_loop(0, SWEEPS - 1, sweep, 0, unroll=levels <= 8)
        for q in range(depth):
            for r in range(2):
                values = [value[f, q, r] for f in range(field_count)]
                for level in range(levels):
                    scale = 1.0 / (levels * root**level)
                    terms = []
                    for mode, real, imag in fields:
                        cosine, sine = wave(levels, mode * level)
                        if imag is None:
                            terms.append((-scale * cosine, values[real]))
                        else:
                            terms.append((-2.0 * scale * cosine, values[real]))
                            terms.append((2.0 * scale * sine, values[imag]))
                    height[level, q, r] = height[level, q, r] + combine(terms)
        return carry

    lax.fori_loop(0, NEWTON, newton, 0)
    for level in range(levels):
        for q in range(depth):
            even, odd = height[level, q, 0], height[level, q, 1]
            rows = pl.ds(q, SUB, stride=depth)
            plain[level, 0, rows, :] = jnp.where(low, even, half_turn(odd))
            plain[level, 1, rows, :] = jnp.where(low, half_turn(even), odd)
    return plain


def newton_kernel(levels, *refs):
    strips, fixed, early, late, halo = refs[:levels], *refs[levels : levels + 4]
    outs = refs[levels + 4 : 2 * levels + 5]
    window, spaces = refs[2 * levels + 5], refs[2 * levels + 6 :]
    strip, keep = fixed.shape[1], late.shape[1]
    me, part = lax.axis_index("tm"), lax.axis_index("sy")
    depth = (HALO + keep) // SUB
    rows = slice(HALO, HALO + keep)
    window[:, :, :HALO] = halo[...]
    lay_taken(levels, window, (1, rows), early, late, slice(0, keep))
    lay(levels, window.at[:, 0], rows, strips, fixed, pl.ds(aligned(part * (strip - keep)), keep))
    plain = newton_steps(levels, lambda field, half, q: window[field, half, pl.ds(q, SUB, stride=depth), :], spaces)
    first = aligned(HALO + part * (keep - strip // 2))
    for shift in range(levels):
        target = lax.rem(me + shift, levels)
        if shift < levels - 1:
            outs[shift][...] = plain[target, :, pl.ds(first, strip // 2)]
        else:
            outs[shift][...] = plain[target, 0, pl.ds(first, strip // 2)]
            outs[shift + 1][...] = plain[target, 1, pl.ds(first, strip // 2)]


def newton_wide_kernel(levels, strip, *refs):
    blocks, outs, spaces = refs[:2], refs[2 : 2 + levels], refs[2 + levels :]
    me = lax.axis_index("tm")
    depth = blocks[0].shape[1] // SUB
    plain = newton_steps(levels, lambda field, half, q: blocks[half][field, pl.ds(q, SUB, stride=depth), :], spaces)
    for shift in range(levels):
        target = lax.rem(me + shift, levels)
        outs[shift][...] = plain[target, 0, HALO : HALO + strip]


def merge_kernel(own, other, out):
    half = own.shape[0]
    part = lax.axis_index("sy")
    out[pl.ds(aligned(part * half), half)] = own[...]
    out[pl.ds(aligned((1 - part) * half), half)] = other[...]


def trade_kernel(*refs):
    out = refs[-1]
    for index, ref in enumerate(refs[:-1]):
        out[index] = ref[1]


def place_kernel(levels, strip, *refs):
    pieces, others, out = refs[:levels], refs[levels:-1], refs[-1]
    part = lax.axis_index("sy")
    cols = out.shape[2]
    lane = lax.broadcasted_iota(jnp.int32, (SUB, cols), 1)
    mixing = lane // 2 + lane % 2 * (cols // 2)

    def put(first, piece):
        for row in range(0, piece.shape[0], SUB):
            out[0, pl.ds(aligned(first + row), SUB)] = pick(piece[row : row + SUB], mixing)

    for shift in range(levels):
        first = strip_of(levels, level_of(levels, shift)) * strip
        if others and shift < levels - 1:
            half = strip // 2
            put(first + part * half, pieces[shift].at[0])
            put(first + (1 - part) * half, others[0].at[shift])
        else:
            put(first, pieces[shift])


def call(kernel, outs, *operands, scratch=(), spec=vmem, params=params):
    return pl.pallas_call(
        kernel,
        out_shape=outs,
        in_specs=[spec] * len(operands),
        out_specs=[vmem] * len(outs) if isinstance(outs, list) else vmem,
        scratch_shapes=list(scratch),
        compiler_params=params,
    )(*operands)


def body(sizes, thickness_guess, thickness_start, bed, rate_factor, mass_balance, cell_flags):
    levels, tiles, parts = sizes
    assert parts == 2
    rows, cols = thickness_start.shape
    strip = rows // levels
    count = 2 * levels + 3
    keep = strip // 2 + HALO

    def swap(value):
        return lax.ppermute(value, "sy", [(0, 1), (1, 0)])

    def around(value, shift):
        return lax.ppermute(value, "tm", [(i, (i + shift) % levels) for i in range(levels)])

    snake = [
        (tm if tile % 2 == 0 else levels - 1 - tm, tile) for tile in range(tiles) for tm in range(levels)
    ]

    def device(place, part):
        tm, tile = snake[place]
        return (tm * tiles + tile) * parts + part

    def along(value, moves):
        pairs = []
        for place in range(len(snake)):
            for part, other, hops in moves:
                if 0 <= place + hops < len(snake):
                    pairs.append((device(place, part), device(place + hops, other)))
        return lax.ppermute(value, ("tm", "sx", "sy"), pairs)

    packed = call(
        functools.partial(pack_kernel, levels, strip),
        [struct(2, strip, cols)] * levels + [struct(3, strip, cols)],
        thickness_guess, mass_balance, thickness_start, bed, rate_factor, cell_flags,
        scratch=(
            pltpu.VMEM((strip, cols), jnp.float32),
            pltpu.VMEM((strip, cols), jnp.int32),
            pltpu.SemaphoreType.DMA((2 * levels + 4,)),
        ),
        spec=hbm,
        params=fetching,
    )
    strips, fixed = packed[:levels], packed[levels]
    strips = [strips[0]] + [around(strips[shift], shift) for shift in range(1, levels)]

    if strip % (2 * SUB) == 0 and keep <= strip:
        def give(*arrays):
            total = sum(array.shape[0] for array in arrays)
            return swap(call(give_kernel, struct(total, keep, cols), *arrays))

        early, late = give(*strips[:-1], fixed), give(strips[-1])
        edge = call(functools.partial(edge_kernel, levels), struct(count, 2, HALO, cols), *strips, fixed, early, late)
        halo = along(edge, [(1, 0, 1), (0, 1, -1)])
        high, half = HALO + keep, strip // 2
        *pieces, own, other = call(
            functools.partial(newton_kernel, levels),
            [struct(2, half, cols)] * (levels - 1) + [struct(half, cols)] * 2,
            *strips, fixed, early, late, halo,
            scratch=[pltpu.VMEM((count, 2, high, cols), jnp.float32)]
            + scratches(levels, high // SUB, cols, high),
        )
        other = swap(other)
        pieces = [pieces[0]] + [around(pieces[shift], shift) for shift in range(1, levels - 1)]
        others = [swap(call(trade_kernel, struct(levels - 1, half, cols), *pieces))]
        pieces.append(around(call(merge_kernel, struct(strip, cols), own, other), levels - 1))
    else:
        counts = [min(strip, HALO - done) for done in range(0, HALO, strip)]
        rims = call(
            functools.partial(rim_kernel, levels, counts),
            [struct(count, n, cols) for n in counts] * 2,
            *strips, fixed,
        )
        aboves = [along(rims[len(counts) + i], [(0, 0, i + 1), (1, 1, i + 1)]) for i in range(len(counts))]
        belows = [along(rims[i], [(0, 0, -i - 1), (1, 1, -i - 1)]) for i in range(len(counts))]
        high = strip + 2 * HALO
        mine = call(
            functools.partial(join_kernel, levels, counts),
            struct(count, high, cols),
            *strips, fixed, *aboves, *belows,
        )
        pieces = call(
            functools.partial(newton_wide_kernel, levels, strip),
            [struct(strip, cols)] * levels,
            mine, swap(mine),
            scratch=scratches(levels, high // SUB, cols, high),
        )
        pieces = [pieces[0]] + [around(pieces[shift], shift) for shift in range(1, levels)]
        others = []
    return call(functools.partial(place_kernel, levels, strip), struct(1, rows, cols), *pieces, *others)


def solution(mesh):
    sizes = tuple(mesh.shape[axis] for axis in ("tm", "sx", "sy"))
    in_specs = (
        P("tm", "sx", "sy"),
        P("sx", "sy"),
        P("sx", "sy"),
        P("sx", "sy"),
        P("tm", "sx", "sy"),
        P("sx", "sy"),
    )
    out_specs = P("tm", "sx", "sy")

    def whole(*args):
        return body(sizes, *args)

    return jax.shard_map(whole, mesh=mesh, in_specs=in_specs, out_specs=out_specs, check_vma=False)
```

```python
import functools
import math

import jax
import jax.numpy as jnp
from jax import lax
from jax.experimental import pallas as pl
from jax.experimental.pallas import tpu as pltpu
from jax.sharding import PartitionSpec as P


NEWTON = 2
SWEEPS = 8
HALO = NEWTON * SWEEPS
SUB = 8

circulant_weight = 0.25
time_step = 1.0


vmem = pl.BlockSpec(memory_space=pltpu.VMEM)
hbm = pl.BlockSpec(memory_space=pltpu.HBM)
params = pltpu.CompilerParams(vmem_limit_bytes=16 * 1024 * 1024)

fetching = pltpu.CompilerParams(vmem_limit_bytes=56125000)


def struct(*shape):
    return jax.ShapeDtypeStruct(shape, jnp.float32)


def aligned(index):
    return pl.multiple_of(index, SUB)


def strip_of(levels, tm):
    return jnp.where(lax.rem(lax.axis_index("sx"), 2) == 0, tm, levels - 1 - tm)


def level_of(levels, shift):
    return lax.rem(lax.axis_index("tm") + levels - shift, levels)


def pick(array, index):
    return jnp.take_along_axis(array, index, axis=1, mode="promise_in_bounds")


def pack_kernel(levels, strip, *refs):
    guess, balance, start, bed, rate, flags = refs[:6]
    strips = refs[6 : 6 + levels]
    fixed, ice, kind, sems = refs[6 + levels :]
    me = lax.axis_index("tm")

    def rows_of(tm):
        return pl.ds(aligned(strip_of(levels, tm) * strip), strip)

    copies = []
    for shift in range(levels):
        here = rows_of(lax.rem(me + shift, levels))
        copies += [(guess.at[0, here], strips[shift].at[0]), (balance.at[0, here], strips[shift].at[1])]
    here = rows_of(me)
    copies += [
        (start.at[here], fixed.at[0]),
        (bed.at[here], fixed.at[1]),
        (rate.at[here], ice),
        (flags.at[here], kind),
    ]
    copies = [pltpu.make_async_copy(a, b, sems.at[i]) for i, (a, b) in enumerate(copies)]
    for copy in copies:
        copy.start()
    for copy in copies:
        copy.wait()
    boost = jnp.where(kind[...] == 2, 2.0, 1.0)
    fixed[2] = jnp.where(kind[...] != 0, boost * ice[...], 0.0)
    cols = fixed.shape[2]
    lane = lax.broadcasted_iota(jnp.int32, (SUB, cols), 1)
    parting = jnp.where(lane < cols // 2, 2 * lane, 2 * lane - (cols - 1))
    for ref in (*strips, fixed):
        for index in range(ref.shape[0]):
            for row in range(0, strip, SUB):
                ref[index, row : row + SUB] = pick(ref[index, row : row + SUB], parting)


def lay(levels, out, rows, strips, fixed, source):
    for shift in range(levels):
        level = level_of(levels, shift)
        out[level, rows] = strips[shift][0, source]
        out[levels + level, rows] = strips[shift][1, source]
    out[2 * levels :, rows] = fixed[:, source]


def give_kernel(*refs):
    out, place = refs[-1], 0
    keep = out.shape[1]
    for ref in refs[:-1]:
        count, strip, _ = ref.shape
        first = aligned((1 - lax.axis_index("sy")) * (strip - keep))
        out[place : place + count] = ref[:, pl.ds(first, keep)]
        place += count


def lay_taken(levels, out, index, early, late, source):
    for shift in range(levels):
        level = level_of(levels, shift)
        ref, place = (early, 2 * shift) if shift < levels - 1 else (late, 0)
        out[(level, *index)] = ref[place, source]
        out[(levels + level, *index)] = ref[place + 1, source]
    out[(slice(2 * levels, None), *index)] = early[2 * levels - 2 :, source]


def edge_kernel(levels, *refs):
    strips, fixed, early, late, out = refs[:levels], *refs[levels:]
    strip, keep = fixed.shape[1], late.shape[1]
    part = lax.axis_index("sy")
    lay_taken(levels, out, (0,), early, late, pl.ds(aligned(part * (keep - HALO)), HALO))
    source = pl.ds(aligned(part * (strip - HALO)), HALO)
    lay(levels, out.at[:, 1], slice(0, HALO), strips, fixed, source)


def rim_kernel(levels, counts, *refs):
    strips = refs[:levels]
    fixed = refs[levels]
    lows, highs = refs[levels + 1 : levels + 1 + len(counts)], refs[levels + 1 + len(counts) :]
    strip = fixed.shape[1]
    for count, low, high in zip(counts, lows, highs):
        lay(levels, low, slice(0, count), strips, fixed, slice(0, count))
        lay(levels, high, slice(0, count), strips, fixed, slice(strip - count, strip))


def join_kernel(levels, counts, *refs):
    strips = refs[:levels]
    fixed = refs[levels]
    aboves, belows = refs[levels + 1 : levels + 1 + len(counts)], refs[levels + 1 + len(counts) : -1]
    out = refs[-1]
    strip = fixed.shape[1]
    lay(levels, out, slice(HALO, HALO + strip), strips, fixed, slice(0, strip))
    done = 0
    for count, above, below in zip(counts, aboves, belows):
        out[:, HALO - done - count : HALO - done] = above[...]
        out[:, HALO + strip + done : HALO + strip + done + count] = below[...]
        done += count


def mode_fields(levels):
    fields, count = [], 0
    for mode in range(levels // 2 + 1):
        if 2 * mode % levels == 0:
            fields.append((mode, count, None))
            count += 1
        else:
            fields.append((mode, count, count + 1))
            count += 2
    return fields, count


def wave(levels, product):
    product %= levels
    quarter = 4 * product
    if quarter % levels == 0:
        return ((1.0, 0.0), (0.0, 1.0), (-1.0, 0.0), (0.0, -1.0))[quarter // levels]
    angle = 2.0 * math.pi * product / levels
    return math.cos(angle), math.sin(angle)


def combine(terms):
    total = None
    for coeff, value in terms:
        if coeff == 0.0:
            continue
        if total is None:
            total = value if coeff == 1.0 else coeff * value
        elif coeff == 1.0:
            total = total + value
        elif coeff == -1.0:
            total = total - value
        else:
            total = total + coeff * value
    return total


def scratches(levels, depth, cols, high):
    _, field_count = mode_fields(levels)
    shapes = [(count, depth, 2, SUB, cols) for count in (levels, levels, 3, levels, 5, *(field_count,) * 4)]
    shapes.append((4, levels, depth, SUB, cols))
    shapes.append((levels, 2, high, cols))
    return [pltpu.VMEM(shape, jnp.float32) for shape in shapes]


def newton_steps(levels, load, spaces):
    height, balance, fixed, diff, weight, inverse, source, value, side, sides, plain = spaces
    depth, _, _, cols = height.shape[1:]
    across = 2 * cols
    lane = lax.broadcasted_iota(jnp.int32, (SUB, cols), 1)
    low = lane < cols // 2
    column = lax.axis_index("sy") * cols
    first = 2 * lane == lax.rem(across - column, across)
    last = 2 * lane + 1 == across - 1 - column
    fields, field_count = mode_fields(levels)
    root = circulant_weight ** (1.0 / levels)

    def half_turn(array):
        return pltpu.roll(array, cols // 2, axis=1)

    def before(odd):
        return pltpu.roll(odd, 1, axis=1)

    def after(even):
        return pltpu.roll(even, cols - 1, axis=1)

    def from_above(array):
        return pltpu.roll(array, 1, axis=0)

    def from_below(array):
        return pltpu.roll(array, SUB - 1, axis=0)

    def rows_around(read):
        blocks = [read(q) for q in range(depth)]
        return [from_above(blocks[-1])] + blocks + [from_below(blocks[0])]

    places = [(height, level, level) for level in range(levels)]
    places += [(balance, level, levels + level) for level in range(levels)]
    places += [(fixed, index, 2 * levels + index) for index in range(3)]
    for ref, index, field in places:
        for q in range(depth):
            left, right = (load(field, half, q) for half in range(2))
            ref[index, q, 0] = jnp.where(low, left, half_turn(right))
            ref[index, q, 1] = jnp.where(low, half_turn(left), right)

    def newton(step, carry):
        for q in range(depth):
            totals = [None] * 4
            for level in range(levels):
                thick = [height[level, q, r] for r in range(2)]
                d = [fixed[2, q, r] * thick[r] * thick[r] * jnp.abs(thick[r]) for r in range(2)]
                s = [thick[r] + fixed[1, q, r] for r in range(2)]
                for r in range(2):
                    diff[level, q, r] = d[r]
                d_left, d_right = jnp.where(first, 0.0, before(d[1])), jnp.where(last, 0.0, after(d[0]))
                sides[0, level, q] = d_left
                sides[1, level, q] = d_right
                sides[2, level, q] = jnp.where(first, 0.0, before(s[1]))
                sides[3, level, q] = jnp.where(last, 0.0, after(s[0]))
                for i, part in enumerate((d[0], d[1], d_left, d_right)):
                    totals[i] = part if level == 0 else totals[i] + part
            even, odd, left, right = (total * (0.5 / levels) for total in totals)
            weight[0, q, 0], weight[0, q, 1] = even, odd
            weight[4, q, 0], weight[4, q, 1] = left, right
        for r in range(2):
            halves = rows_around(lambda q: weight[0, q, r])
            downs = [halves[q] + halves[q + 1] for q in range(depth + 1)]
            others = [weight[0, q, 1 - r] for q in range(depth)]
            for q in range(depth):
                here, up, down = halves[q + 1], downs[q], downs[q + 1]
                inner, outer = here + others[q], here + weight[4, q, r]
                weight[1, q, r] = up
                weight[2, q, r] = down
                if r == 0:
                    weight[3, q, 0] = inner
                weight[4, q, r] = jnp.where(last if r else first, 0.0, outer)
                total = (up + down) + (inner + outer)
                inside = jnp.where(fixed[2, q, r] > 0.0, 1.0, 0.0)
                for mode, real, imag in fields:
                    cosine, sine = wave(levels, mode)
                    denom = total + (1.0 - root * cosine) / time_step
                    if imag is None:
                        inverse[real, q, r] = inside / denom
                    else:
                        shift = root * sine / time_step
                        ratio = inside / (denom * denom + shift * shift)
                        inverse[real, q, r] = ratio * denom
                        inverse[imag, q, r] = ratio * -shift
        for level in range(levels):
            ds, ss, inners = [], [], []
            for r in range(2):
                ds.append(rows_around(lambda q: diff[level, q, r]))
                ss.append(rows_around(lambda q: height[level, q, r] + fixed[1, q, r]))
            for q in range(depth):
                inners.append((ds[0][q + 1] + ds[1][q + 1]) * (ss[0][q + 1] - ss[1][q + 1]))
            for r in range(2):
                d, s = ds[r], ss[r]
                downs = [(d[q] + d[q + 1]) * (s[q] - s[q + 1]) for q in range(depth + 1)]
                for q in range(depth):
                    outer = (d[q + 1] + sides[r, level, q]) * (s[q + 1] - sides[2 + r, level, q])
                    across_flux = outer - inners[q] if r else outer + inners[q]
                    prior = height[level - 1, q, r] if level > 0 else fixed[0, q, r]
                    change = (
                        (height[level, q, r] - prior) / time_step
                        + 0.5 * ((downs[q + 1] - downs[q]) + across_flux)
                        - balance[level, q, r]
                    )
                    scaled = change if level == 0 else change * root**level
                    source_part = jnp.where(fixed[2, q, r] > 0.0, scaled, 0.0)
                    diff[level, q, r] = source_part

        def put(f, q, parts):
            value[f, q, 0], value[f, q, 1] = parts
            side[f, q, 0], side[f, q, 1] = before(parts[1]), after(parts[0])

        for q in range(depth):
            scaled = [[diff[level, q, r] for level in range(levels)] for r in range(2)]
            for mode, real, imag in fields:
                waves = [wave(levels, mode * level) for level in range(levels)]
                y_real = [combine([(w[0], v) for w, v in zip(waves, scaled[r])]) for r in range(2)]
                i_real = [inverse[real, q, r] for r in range(2)]
                for r in range(2):
                    source[real, q, r] = y_real[r]
                if imag is None:
                    put(real, q, [i_real[r] * y_real[r] for r in range(2)])
                else:
                    y_imag = [combine([(-w[1], v) for w, v in zip(waves, scaled[r])]) for r in range(2)]
                    i_imag = [inverse[imag, q, r] for r in range(2)]
                    for r in range(2):
                        source[imag, q, r] = y_imag[r]
                    put(real, q, [y_real[r] * i_real[r] - y_imag[r] * i_imag[r] for r in range(2)])
                    put(imag, q, [y_real[r] * i_imag[r] + y_imag[r] * i_real[r] for r in range(2)])

        def sweep(index, carry):
            tops = [[value[f, 0, r] for r in range(2)] for f in range(field_count)]
            befores = [[from_above(value[f, depth - 1, r]) for r in range(2)] for f in range(field_count)]
            heres = tops
            for q in range(depth):
                inner = weight[3, q, 0]
                numer, nexts = [], []
                for f in range(field_count):
                    if q + 1 < depth:
                        nexts.append([value[f, q + 1, r] for r in range(2)])
                    else:
                        nexts.append([from_below(tops[f][r]) for r in range(2)])
                    numer.append([
                        source[f, q, r]
                        + ((weight[1, q, r] * befores[f][r] + weight[2, q, r] * nexts[f][r])
                        + (inner * heres[f][1 - r] + weight[4, q, r] * side[f, q, r]))
                        for r in range(2)
                    ])
                for mode, real, imag in fields:
                    i_real = [inverse[real, q, r] for r in range(2)]
                    if imag is None:
                        put(real, q, [i_real[r] * numer[real][r] for r in range(2)])
                    else:
                        i_imag = [inverse[imag, q, r] for r in range(2)]
                        put(real, q, [numer[real][r] * i_real[r] - numer[imag][r] * i_imag[r] for r in range(2)])
                        put(imag, q, [numer[real][r] * i_imag[r] + numer[imag][r] * i_real[r] for r in range(2)])
                befores, heres = heres, nexts
            return carry

        lax.fori_loop(0, SWEEPS - 1, sweep, 0, unroll=levels <= 8)
        for q in range(depth):
            for r in range(2):
                values = [value[f, q, r] for f in range(field_count)]
                for level in range(levels):
                    scale = 1.0 / (levels * root**level)
                    terms = []
                    for mode, real, imag in fields:
                        cosine, sine = wave(levels, mode * level)
                        if imag is None:
                            terms.append((-scale * cosine, values[real]))
                        else:
                            terms.append((-2.0 * scale * cosine, values[real]))
                            terms.append((2.0 * scale * sine, values[imag]))
                    height[level, q, r] = height[level, q, r] + combine(terms)
        return carry

    lax.fori_loop(0, NEWTON, newton, 0)
    for level in range(levels):
        for q in range(depth):
            even, odd = height[level, q, 0], height[level, q, 1]
            rows = pl.ds(q, SUB, stride=depth)
            plain[level, 0, rows, :] = jnp.where(low, even, half_turn(odd))
            plain[level, 1, rows, :] = jnp.where(low, half_turn(even), odd)
    return plain


def newton_kernel(levels, *refs):
    strips, fixed, early, late, halo = refs[:levels], *refs[levels : levels + 4]
    spaces = refs[levels + 4 :]
    outs, window, spaces = spaces[: levels - ahead(levels) + 2], spaces[levels - ahead(levels) + 2], spaces[levels - ahead(levels) + 3 :]
    strip, keep = fixed.shape[1], late.shape[1]
    me, part = lax.axis_index("tm"), lax.axis_index("sy")
    depth = (HALO + keep) // SUB
    rows = slice(HALO, HALO + keep)
    window[:, :, :HALO] = halo[...]
    lay_taken(levels, window, (1, rows), early, late, slice(0, keep))
    lay(levels, window.at[:, 0], rows, strips, fixed, pl.ds(aligned(part * (strip - keep)), keep))
    plain = newton_steps(levels, lambda field, half, q: window[field, half, pl.ds(q, SUB, stride=depth), :], spaces)
    first = aligned(HALO + part * (keep - strip // 2))
    early = levels - ahead(levels)
    own, other = outs[early:]
    for shift in range(levels):
        target = lax.rem(me + shift, levels)
        if shift < early:
            outs[shift][...] = plain[target, :, pl.ds(first, strip // 2)]
        else:
            own[shift - early] = plain[target, 0, pl.ds(first, strip // 2)]
            other[shift - early] = plain[target, 1, pl.ds(first, strip // 2)]


def newton_wide_kernel(levels, strip, *refs):
    blocks, outs, spaces = refs[:2], refs[2 : 2 + levels], refs[2 + levels :]
    me = lax.axis_index("tm")
    depth = blocks[0].shape[1] // SUB
    plain = newton_steps(levels, lambda field, half, q: blocks[half][field, pl.ds(q, SUB, stride=depth), :], spaces)
    for shift in range(levels):
        target = lax.rem(me + shift, levels)
        outs[shift][...] = plain[target, 0, HALO : HALO + strip]


def ahead(levels):
    return max(1, levels // 2)


def merge_kernel(own, other, *outs):
    half = own.shape[1]
    part = lax.axis_index("sy")
    for index, out in enumerate(outs):
        out[pl.ds(aligned(part * half), half)] = own[index]
        out[pl.ds(aligned((1 - part) * half), half)] = other[index]


def trade_kernel(*refs):
    out = refs[-1]
    for index, ref in enumerate(refs[:-1]):
        out[index] = ref[1]


def place_kernel(levels, strip, *refs):
    pieces, others, out = refs[:levels], refs[levels:-1], refs[-1]
    part = lax.axis_index("sy")
    cols = out.shape[2]
    lane = lax.broadcasted_iota(jnp.int32, (SUB, cols), 1)
    mixing = lane // 2 + lane % 2 * (cols // 2)

    def put(first, piece):
        for row in range(0, piece.shape[0], SUB):
            out[0, pl.ds(aligned(first + row), SUB)] = pick(piece[row : row + SUB], mixing)

    for shift in range(levels):
        first = strip_of(levels, level_of(levels, shift)) * strip
        if others and shift < levels - ahead(levels):
            half = strip // 2
            put(first + part * half, pieces[shift].at[0])
            put(first + (1 - part) * half, others[0].at[shift])
        else:
            put(first, pieces[shift])


def call(kernel, outs, *operands, scratch=(), spec=vmem, params=params):
    return pl.pallas_call(
        kernel,
        out_shape=outs,
        in_specs=[spec] * len(operands),
        out_specs=[vmem] * len(outs) if isinstance(outs, list) else vmem,
        scratch_shapes=list(scratch),
        compiler_params=params,
    )(*operands)


def body(sizes, thickness_guess, thickness_start, bed, rate_factor, mass_balance, cell_flags):
    levels, tiles, parts = sizes
    assert parts == 2
    rows, cols = thickness_start.shape
    strip = rows // levels
    count = 2 * levels + 3
    keep = strip // 2 + HALO

    def swap(value):
        return lax.ppermute(value, "sy", [(0, 1), (1, 0)])

    def around(value, shift):
        return lax.ppermute(value, "tm", [(i, (i + shift) % levels) for i in range(levels)])

    snake = [
        (tm if tile % 2 == 0 else levels - 1 - tm, tile) for tile in range(tiles) for tm in range(levels)
    ]

    def device(place, part):
        tm, tile = snake[place]
        return (tm * tiles + tile) * parts + part

    def along(value, moves):
        pairs = []
        for place in range(len(snake)):
            for part, other, hops in moves:
                if 0 <= place + hops < len(snake):
                    pairs.append((device(place, part), device(place + hops, other)))
        return lax.ppermute(value, ("tm", "sx", "sy"), pairs)

    packed = call(
        functools.partial(pack_kernel, levels, strip),
        [struct(2, strip, cols)] * levels + [struct(3, strip, cols)],
        thickness_guess, mass_balance, thickness_start, bed, rate_factor, cell_flags,
        scratch=(
            pltpu.VMEM((strip, cols), jnp.float32),
            pltpu.VMEM((strip, cols), jnp.int32),
            pltpu.SemaphoreType.DMA((2 * levels + 4,)),
        ),
        spec=hbm,
        params=fetching,
    )
    strips, fixed = packed[:levels], packed[levels]
    strips = [strips[0]] + [around(strips[shift], shift) for shift in range(1, levels)]

    if strip % (2 * SUB) == 0 and keep <= strip:
        def give(*arrays):
            total = sum(array.shape[0] for array in arrays)
            return swap(call(give_kernel, struct(total, keep, cols), *arrays))

        first, second = give(*strips[:-1], fixed), give(strips[-1])
        edge = call(functools.partial(edge_kernel, levels), struct(count, 2, HALO, cols), *strips, fixed, first, second)
        halo = along(edge, [(1, 0, 1), (0, 1, -1)])
        high, half, late = HALO + keep, strip // 2, ahead(levels)
        *pieces, own, other = call(
            functools.partial(newton_kernel, levels),
            [struct(2, half, cols)] * (levels - late) + [struct(late, half, cols)] * 2,
            *strips, fixed, first, second, halo,
            scratch=[pltpu.VMEM((count, 2, high, cols), jnp.float32)]
            + scratches(levels, high // SUB, cols, high),
        )
        other = swap(other)
        early = levels - late
        pieces = [pieces[0]] + [around(pieces[shift], shift) for shift in range(1, early)]
        others = [swap(call(trade_kernel, struct(early, half, cols), *pieces))]
        merged = call(merge_kernel, [struct(strip, cols)] * late, own, other)
        pieces += [around(piece, shift) for shift, piece in enumerate(merged, early)]
    else:
        counts = [min(strip, HALO - done) for done in range(0, HALO, strip)]
        rims = call(
            functools.partial(rim_kernel, levels, counts),
            [struct(count, n, cols) for n in counts] * 2,
            *strips, fixed,
        )
        aboves = [along(rims[len(counts) + i], [(0, 0, i + 1), (1, 1, i + 1)]) for i in range(len(counts))]
        belows = [along(rims[i], [(0, 0, -i - 1), (1, 1, -i - 1)]) for i in range(len(counts))]
        high = strip + 2 * HALO
        mine = call(
            functools.partial(join_kernel, levels, counts),
            struct(count, high, cols),
            *strips, fixed, *aboves, *belows,
        )
        pieces = call(
            functools.partial(newton_wide_kernel, levels, strip),
            [struct(strip, cols)] * levels,
            mine, swap(mine),
            scratch=scratches(levels, high // SUB, cols, high),
        )
        pieces = [pieces[0]] + [around(pieces[shift], shift) for shift in range(1, levels)]
        others = []
    return call(functools.partial(place_kernel, levels, strip), struct(1, rows, cols), *pieces, *others)


def solution(mesh):
    sizes = tuple(mesh.shape[axis] for axis in ("tm", "sx", "sy"))
    in_specs = (
        P("tm", "sx", "sy"),
        P("sx", "sy"),
        P("sx", "sy"),
        P("sx", "sy"),
        P("tm", "sx", "sy"),
        P("sx", "sy"),
    )
    out_specs = P("tm", "sx", "sy")

    def whole(*args):
        return body(sizes, *args)

    return jax.shard_map(whole, mesh=mesh, in_specs=in_specs, out_specs=out_specs, check_vma=False)
```

```python
import functools
import math

import jax
import jax.numpy as jnp
from jax import lax
from jax.experimental import pallas as pl
from jax.experimental.pallas import tpu as pltpu
from jax.sharding import PartitionSpec as P


NEWTON = 2
SWEEPS = 8
HALO = NEWTON * SWEEPS
SUB = 8

circulant_weight = 0.25
time_step = 1.0


vmem = pl.BlockSpec(memory_space=pltpu.VMEM)
hbm = pl.BlockSpec(memory_space=pltpu.HBM)
params = pltpu.CompilerParams(vmem_limit_bytes=16 * 1024 * 1024)

fetching = pltpu.CompilerParams(vmem_limit_bytes=56125000)


def struct(*shape):
    return jax.ShapeDtypeStruct(shape, jnp.float32)


def aligned(index):
    return pl.multiple_of(index, SUB)


def strip_of(levels, tm):
    return jnp.where(lax.rem(lax.axis_index("sx"), 2) == 0, tm, levels - 1 - tm)


def way_out(levels):
    return [*range(levels - 2), levels - 1, levels - 2] if levels > 2 else list(range(levels))


def level_of(levels, shift):
    return lax.rem(lax.axis_index("tm") + levels - shift, levels)


def pick(array, index):
    return jnp.take_along_axis(array, index, axis=1, mode="promise_in_bounds")


def pack_kernel(levels, strip, *refs):
    guess, balance, start, bed, rate, flags = refs[:6]
    strips = refs[6 : 6 + levels]
    fixed, ice, kind, sems = refs[6 + levels :]
    me = lax.axis_index("tm")

    def rows_of(tm):
        return pl.ds(aligned(strip_of(levels, tm) * strip), strip)

    copies = []
    for shift in range(levels):
        here = rows_of(lax.rem(me + way_out(levels)[shift], levels))
        copies += [(guess.at[0, here], strips[shift].at[0]), (balance.at[0, here], strips[shift].at[1])]
    here = rows_of(me)
    copies += [
        (start.at[here], fixed.at[0]),
        (bed.at[here], fixed.at[1]),
        (rate.at[here], ice),
        (flags.at[here], kind),
    ]
    copies = [pltpu.make_async_copy(a, b, sems.at[i]) for i, (a, b) in enumerate(copies)]
    for copy in copies:
        copy.start()
    for copy in copies:
        copy.wait()
    boost = jnp.where(kind[...] == 2, 2.0, 1.0)
    fixed[2] = jnp.where(kind[...] != 0, boost * ice[...], 0.0)
    cols = fixed.shape[2]
    lane = lax.broadcasted_iota(jnp.int32, (SUB, cols), 1)
    parting = jnp.where(lane < cols // 2, 2 * lane, 2 * lane - (cols - 1))
    for ref in (*strips, fixed):
        for index in range(ref.shape[0]):
            for row in range(0, strip, SUB):
                ref[index, row : row + SUB] = pick(ref[index, row : row + SUB], parting)


def lay(levels, out, rows, strips, fixed, source):
    for shift, hops in enumerate(way_out(levels)):
        level = level_of(levels, hops)
        out[level, rows] = strips[shift][0, source]
        out[levels + level, rows] = strips[shift][1, source]
    out[2 * levels :, rows] = fixed[:, source]


def give_kernel(*refs):
    out, place = refs[-1], 0
    keep = out.shape[1]
    for ref in refs[:-1]:
        count, strip, _ = ref.shape
        first = aligned((1 - lax.axis_index("sy")) * (strip - keep))
        out[place : place + count] = ref[:, pl.ds(first, keep)]
        place += count


def lay_taken(levels, out, index, early, late, source):
    for shift, hops in enumerate(way_out(levels)):
        level = level_of(levels, hops)
        ref, place = (early, 2 * shift) if shift < levels - 1 else (late, 0)
        out[(level, *index)] = ref[place, source]
        out[(levels + level, *index)] = ref[place + 1, source]
    out[(slice(2 * levels, None), *index)] = early[2 * levels - 2 :, source]


def edge_kernel(levels, *refs):
    strips, fixed, early, late, out = refs[:levels], *refs[levels:]
    strip, keep = fixed.shape[1], late.shape[1]
    part = lax.axis_index("sy")
    lay_taken(levels, out, (0,), early, late, pl.ds(aligned(part * (keep - HALO)), HALO))
    source = pl.ds(aligned(part * (strip - HALO)), HALO)
    lay(levels, out.at[:, 1], slice(0, HALO), strips, fixed, source)


def rim_kernel(levels, counts, *refs):
    strips = refs[:levels]
    fixed = refs[levels]
    lows, highs = refs[levels + 1 : levels + 1 + len(counts)], refs[levels + 1 + len(counts) :]
    strip = fixed.shape[1]
    for count, low, high in zip(counts, lows, highs):
        lay(levels, low, slice(0, count), strips, fixed, slice(0, count))
        lay(levels, high, slice(0, count), strips, fixed, slice(strip - count, strip))


def join_kernel(levels, counts, *refs):
    strips = refs[:levels]
    fixed = refs[levels]
    aboves, belows = refs[levels + 1 : levels + 1 + len(counts)], refs[levels + 1 + len(counts) : -1]
    out = refs[-1]
    strip = fixed.shape[1]
    lay(levels, out, slice(HALO, HALO + strip), strips, fixed, slice(0, strip))
    done = 0
    for count, above, below in zip(counts, aboves, belows):
        out[:, HALO - done - count : HALO - done] = above[...]
        out[:, HALO + strip + done : HALO + strip + done + count] = below[...]
        done += count


def mode_fields(levels):
    fields, count = [], 0
    for mode in range(levels // 2 + 1):
        if 2 * mode % levels == 0:
            fields.append((mode, count, None))
            count += 1
        else:
            fields.append((mode, count, count + 1))
            count += 2
    return fields, count


def wave(levels, product):
    product %= levels
    quarter = 4 * product
    if quarter % levels == 0:
        return ((1.0, 0.0), (0.0, 1.0), (-1.0, 0.0), (0.0, -1.0))[quarter // levels]
    angle = 2.0 * math.pi * product / levels
    return math.cos(angle), math.sin(angle)


def combine(terms):
    total = None
    for coeff, value in terms:
        if coeff == 0.0:
            continue
        if total is None:
            total = value if coeff == 1.0 else coeff * value
        elif coeff == 1.0:
            total = total + value
        elif coeff == -1.0:
            total = total - value
        else:
            total = total + coeff * value
    return total


def scratches(levels, depth, cols, high):
    _, field_count = mode_fields(levels)
    shapes = [(count, depth, 2, SUB, cols) for count in (levels, levels, 3, levels, 5, *(field_count,) * 4)]
    shapes.append((4, levels, depth, SUB, cols))
    shapes.append((levels, 2, high, cols))
    return [pltpu.VMEM(shape, jnp.float32) for shape in shapes]


def newton_steps(levels, load, spaces):
    height, balance, fixed, diff, weight, inverse, source, value, side, sides, plain = spaces
    depth, _, _, cols = height.shape[1:]
    across = 2 * cols
    lane = lax.broadcasted_iota(jnp.int32, (SUB, cols), 1)
    low = lane < cols // 2
    column = lax.axis_index("sy") * cols
    first = 2 * lane == lax.rem(across - column, across)
    last = 2 * lane + 1 == across - 1 - column
    fields, field_count = mode_fields(levels)
    root = circulant_weight ** (1.0 / levels)

    def half_turn(array):
        return pltpu.roll(array, cols // 2, axis=1)

    def before(odd):
        return pltpu.roll(odd, 1, axis=1)

    def after(even):
        return pltpu.roll(even, cols - 1, axis=1)

    def from_above(array):
        return pltpu.roll(array, 1, axis=0)

    def from_below(array):
        return pltpu.roll(array, SUB - 1, axis=0)

    def rows_around(read):
        blocks = [read(q) for q in range(depth)]
        return [from_above(blocks[-1])] + blocks + [from_below(blocks[0])]

    places = [(height, level, level) for level in range(levels)]
    places += [(balance, level, levels + level) for level in range(levels)]
    places += [(fixed, index, 2 * levels + index) for index in range(3)]
    for ref, index, field in places:
        for q in range(depth):
            left, right = (load(field, half, q) for half in range(2))
            ref[index, q, 0] = jnp.where(low, left, half_turn(right))
            ref[index, q, 1] = jnp.where(low, half_turn(left), right)

    def newton(step, carry):
        for q in range(depth):
            totals = [None] * 4
            for level in range(levels):
                thick = [height[level, q, r] for r in range(2)]
                d = [fixed[2, q, r] * thick[r] * thick[r] * jnp.abs(thick[r]) for r in range(2)]
                s = [thick[r] + fixed[1, q, r] for r in range(2)]
                for r in range(2):
                    diff[level, q, r] = d[r]
                d_left, d_right = jnp.where(first, 0.0, before(d[1])), jnp.where(last, 0.0, after(d[0]))
                sides[0, level, q] = d_left
                sides[1, level, q] = d_right
                sides[2, level, q] = jnp.where(first, 0.0, before(s[1]))
                sides[3, level, q] = jnp.where(last, 0.0, after(s[0]))
                for i, part in enumerate((d[0], d[1], d_left, d_right)):
                    totals[i] = part if level == 0 else totals[i] + part
            even, odd, left, right = (total * (0.5 / levels) for total in totals)
            weight[0, q, 0], weight[0, q, 1] = even, odd
            weight[4, q, 0], weight[4, q, 1] = left, right
        for r in range(2):
            halves = rows_around(lambda q: weight[0, q, r])
            downs = [halves[q] + halves[q + 1] for q in range(depth + 1)]
            others = [weight[0, q, 1 - r] for q in range(depth)]
            for q in range(depth):
                here, up, down = halves[q + 1], downs[q], downs[q + 1]
                inner, outer = here + others[q], here + weight[4, q, r]
                weight[1, q, r] = up
                weight[2, q, r] = down
                if r == 0:
                    weight[3, q, 0] = inner
                weight[4, q, r] = jnp.where(last if r else first, 0.0, outer)
                total = (up + down) + (inner + outer)
                inside = jnp.where(fixed[2, q, r] > 0.0, 1.0, 0.0)
                for mode, real, imag in fields:
                    cosine, sine = wave(levels, mode)
                    denom = total + (1.0 - root * cosine) / time_step
                    if imag is None:
                        inverse[real, q, r] = inside / denom
                    else:
                        shift = root * sine / time_step
                        ratio = inside / (denom * denom + shift * shift)
                        inverse[real, q, r] = ratio * denom
                        inverse[imag, q, r] = ratio * -shift
        for level in range(levels):
            ds, ss, inners = [], [], []
            for r in range(2):
                ds.append(rows_around(lambda q: diff[level, q, r]))
                ss.append(rows_around(lambda q: height[level, q, r] + fixed[1, q, r]))
            for q in range(depth):
                inners.append((ds[0][q + 1] + ds[1][q + 1]) * (ss[0][q + 1] - ss[1][q + 1]))
            for r in range(2):
                d, s = ds[r], ss[r]
                downs = [(d[q] + d[q + 1]) * (s[q] - s[q + 1]) for q in range(depth + 1)]
                for q in range(depth):
                    outer = (d[q + 1] + sides[r, level, q]) * (s[q + 1] - sides[2 + r, level, q])
                    across_flux = outer - inners[q] if r else outer + inners[q]
                    prior = height[level - 1, q, r] if level > 0 else fixed[0, q, r]
                    change = (
                        (height[level, q, r] - prior) / time_step
                        + 0.5 * ((downs[q + 1] - downs[q]) + across_flux)
                        - balance[level, q, r]
                    )
                    scaled = change if level == 0 else change * root**level
                    source_part = jnp.where(fixed[2, q, r] > 0.0, scaled, 0.0)
                    diff[level, q, r] = source_part

        def put(f, q, parts):
            value[f, q, 0], value[f, q, 1] = parts
            side[f, q, 0], side[f, q, 1] = before(parts[1]), after(parts[0])

        for q in range(depth):
            scaled = [[diff[level, q, r] for level in range(levels)] for r in range(2)]
            for mode, real, imag in fields:
                waves = [wave(levels, mode * level) for level in range(levels)]
                y_real = [combine([(w[0], v) for w, v in zip(waves, scaled[r])]) for r in range(2)]
                i_real = [inverse[real, q, r] for r in range(2)]
                for r in range(2):
                    source[real, q, r] = y_real[r]
                if imag is None:
                    put(real, q, [i_real[r] * y_real[r] for r in range(2)])
                else:
                    y_imag = [combine([(-w[1], v) for w, v in zip(waves, scaled[r])]) for r in range(2)]
                    i_imag = [inverse[imag, q, r] for r in range(2)]
                    for r in range(2):
                        source[imag, q, r] = y_imag[r]
                    put(real, q, [y_real[r] * i_real[r] - y_imag[r] * i_imag[r] for r in range(2)])
                    put(imag, q, [y_real[r] * i_imag[r] + y_imag[r] * i_real[r] for r in range(2)])

        def sweep(index, carry):
            tops = [[value[f, 0, r] for r in range(2)] for f in range(field_count)]
            befores = [[from_above(value[f, depth - 1, r]) for r in range(2)] for f in range(field_count)]
            heres = tops
            for q in range(depth):
                inner = weight[3, q, 0]
                numer, nexts = [], []
                for f in range(field_count):
                    if q + 1 < depth:
                        nexts.append([value[f, q + 1, r] for r in range(2)])
                    else:
                        nexts.append([from_below(tops[f][r]) for r in range(2)])
                    numer.append([
                        source[f, q, r]
                        + ((weight[1, q, r] * befores[f][r] + weight[2, q, r] * nexts[f][r])
                        + (inner * heres[f][1 - r] + weight[4, q, r] * side[f, q, r]))
                        for r in range(2)
                    ])
                for mode, real, imag in fields:
                    i_real = [inverse[real, q, r] for r in range(2)]
                    if imag is None:
                        put(real, q, [i_real[r] * numer[real][r] for r in range(2)])
                    else:
                        i_imag = [inverse[imag, q, r] for r in range(2)]
                        put(real, q, [numer[real][r] * i_real[r] - numer[imag][r] * i_imag[r] for r in range(2)])
                        put(imag, q, [numer[real][r] * i_imag[r] + numer[imag][r] * i_real[r] for r in range(2)])
                befores, heres = heres, nexts
            return carry

        lax.fori_loop(0, SWEEPS - 1, sweep, 0, unroll=levels <= 8)
        for q in range(depth):
            for r in range(2):
                values = [value[f, q, r] for f in range(field_count)]
                for level in range(levels):
                    scale = 1.0 / (levels * root**level)
                    terms = []
                    for mode, real, imag in fields:
                        cosine, sine = wave(levels, mode * level)
                        if imag is None:
                            terms.append((-scale * cosine, values[real]))
                        else:
                            terms.append((-2.0 * scale * cosine, values[real]))
                            terms.append((2.0 * scale * sine, values[imag]))
                    height[level, q, r] = height[level, q, r] + combine(terms)
        return carry

    lax.fori_loop(0, NEWTON, newton, 0)
    for level in range(levels):
        for q in range(depth):
            even, odd = height[level, q, 0], height[level, q, 1]
            rows = pl.ds(q, SUB, stride=depth)
            plain[level, 0, rows, :] = jnp.where(low, even, half_turn(odd))
            plain[level, 1, rows, :] = jnp.where(low, half_turn(even), odd)
    return plain


def newton_kernel(levels, *refs):
    strips, fixed, early, late, halo = refs[:levels], *refs[levels : levels + 4]
    spaces = refs[levels + 4 :]
    outs, window, spaces = spaces[: levels - ahead(levels) + 2], spaces[levels - ahead(levels) + 2], spaces[levels - ahead(levels) + 3 :]
    strip, keep = fixed.shape[1], late.shape[1]
    me, part = lax.axis_index("tm"), lax.axis_index("sy")
    depth = (HALO + keep) // SUB
    rows = slice(HALO, HALO + keep)
    window[:, :, :HALO] = halo[...]
    lay_taken(levels, window, (1, rows), early, late, slice(0, keep))
    lay(levels, window.at[:, 0], rows, strips, fixed, pl.ds(aligned(part * (strip - keep)), keep))
    plain = newton_steps(levels, lambda field, half, q: window[field, half, pl.ds(q, SUB, stride=depth), :], spaces)
    first = aligned(HALO + part * (keep - strip // 2))
    early = levels - ahead(levels)
    own, other = outs[early:]
    for shift in range(levels):
        target = lax.rem(me + shift, levels)
        if shift < early:
            outs[shift][...] = plain[target, :, pl.ds(first, strip // 2)]
        else:
            own[shift - early] = plain[target, 0, pl.ds(first, strip // 2)]
            other[shift - early] = plain[target, 1, pl.ds(first, strip // 2)]


def newton_wide_kernel(levels, strip, *refs):
    blocks, outs, spaces = refs[:2], refs[2 : 2 + levels], refs[2 + levels :]
    me = lax.axis_index("tm")
    depth = blocks[0].shape[1] // SUB
    plain = newton_steps(levels, lambda field, half, q: blocks[half][field, pl.ds(q, SUB, stride=depth), :], spaces)
    for shift in range(levels):
        target = lax.rem(me + shift, levels)
        outs[shift][...] = plain[target, 0, HALO : HALO + strip]


def ahead(levels):
    return max(1, levels // 2)


def merge_kernel(own, other, *outs):
    half = own.shape[1]
    part = lax.axis_index("sy")
    for index, out in enumerate(outs):
        out[pl.ds(aligned(part * half), half)] = own[index]
        out[pl.ds(aligned((1 - part) * half), half)] = other[index]


def trade_kernel(*refs):
    out = refs[-1]
    for index, ref in enumerate(refs[:-1]):
        out[index] = ref[1]


def place_kernel(levels, strip, *refs):
    pieces, others, out = refs[:levels], refs[levels:-1], refs[-1]
    part = lax.axis_index("sy")
    cols = out.shape[2]
    lane = lax.broadcasted_iota(jnp.int32, (SUB, cols), 1)
    mixing = lane // 2 + lane % 2 * (cols // 2)

    def put(first, piece):
        for row in range(0, piece.shape[0], SUB):
            out[0, pl.ds(aligned(first + row), SUB)] = pick(piece[row : row + SUB], mixing)

    for shift in range(levels):
        first = strip_of(levels, level_of(levels, shift)) * strip
        if others and shift < levels - ahead(levels):
            half = strip // 2
            put(first + part * half, pieces[shift].at[0])
            put(first + (1 - part) * half, others[0].at[shift])
        else:
            put(first, pieces[shift])


def call(kernel, outs, *operands, scratch=(), spec=vmem, params=params):
    return pl.pallas_call(
        kernel,
        out_shape=outs,
        in_specs=[spec] * len(operands),
        out_specs=[vmem] * len(outs) if isinstance(outs, list) else vmem,
        scratch_shapes=list(scratch),
        compiler_params=params,
    )(*operands)


def body(sizes, thickness_guess, thickness_start, bed, rate_factor, mass_balance, cell_flags):
    levels, tiles, parts = sizes
    assert parts == 2
    rows, cols = thickness_start.shape
    strip = rows // levels
    count = 2 * levels + 3
    keep = strip // 2 + HALO

    def swap(value):
        return lax.ppermute(value, "sy", [(0, 1), (1, 0)])

    def around(value, shift):
        return lax.ppermute(value, "tm", [(i, (i + shift) % levels) for i in range(levels)])

    snake = [
        (tm if tile % 2 == 0 else levels - 1 - tm, tile) for tile in range(tiles) for tm in range(levels)
    ]

    def device(place, part):
        tm, tile = snake[place]
        return (tm * tiles + tile) * parts + part

    def along(value, moves):
        pairs = []
        for place in range(len(snake)):
            for part, other, hops in moves:
                if 0 <= place + hops < len(snake):
                    pairs.append((device(place, part), device(place + hops, other)))
        return lax.ppermute(value, ("tm", "sx", "sy"), pairs)

    packed = call(
        functools.partial(pack_kernel, levels, strip),
        [struct(2, strip, cols)] * levels + [struct(3, strip, cols)],
        thickness_guess, mass_balance, thickness_start, bed, rate_factor, cell_flags,
        scratch=(
            pltpu.VMEM((strip, cols), jnp.float32),
            pltpu.VMEM((strip, cols), jnp.int32),
            pltpu.SemaphoreType.DMA((2 * levels + 4,)),
        ),
        spec=hbm,
        params=fetching,
    )
    strips, fixed = packed[:levels], packed[levels]
    hops = way_out(levels)
    strips = [strips[0]] + [around(strips[turn], hops[turn]) for turn in range(1, levels)]

    if strip % (2 * SUB) == 0 and keep <= strip:
        def give(*arrays):
            total = sum(array.shape[0] for array in arrays)
            return swap(call(give_kernel, struct(total, keep, cols), *arrays))

        first, second = give(*strips[:-1], fixed), give(strips[-1])
        edge = call(functools.partial(edge_kernel, levels), struct(count, 2, HALO, cols), *strips, fixed, first, second)
        halo = along(edge, [(1, 0, 1), (0, 1, -1)])
        high, half, late = HALO + keep, strip // 2, ahead(levels)
        *pieces, own, other = call(
            functools.partial(newton_kernel, levels),
            [struct(2, half, cols)] * (levels - late) + [struct(late, half, cols)] * 2,
            *strips, fixed, first, second, halo,
            scratch=[pltpu.VMEM((count, 2, high, cols), jnp.float32)]
            + scratches(levels, high // SUB, cols, high),
        )
        other = swap(other)
        early = levels - late
        pieces = [pieces[0]] + [around(pieces[shift], shift) for shift in range(1, early)]
        others = [swap(call(trade_kernel, struct(early, half, cols), *pieces))]
        merged = call(merge_kernel, [struct(strip, cols)] * late, own, other)
        pieces += [around(piece, shift) for shift, piece in enumerate(merged, early)]
    else:
        counts = [min(strip, HALO - done) for done in range(0, HALO, strip)]
        rims = call(
            functools.partial(rim_kernel, levels, counts),
            [struct(count, n, cols) for n in counts] * 2,
            *strips, fixed,
        )
        aboves = [along(rims[len(counts) + i], [(0, 0, i + 1), (1, 1, i + 1)]) for i in range(len(counts))]
        belows = [along(rims[i], [(0, 0, -i - 1), (1, 1, -i - 1)]) for i in range(len(counts))]
        high = strip + 2 * HALO
        mine = call(
            functools.partial(join_kernel, levels, counts),
            struct(count, high, cols),
            *strips, fixed, *aboves, *belows,
        )
        pieces = call(
            functools.partial(newton_wide_kernel, levels, strip),
            [struct(strip, cols)] * levels,
            mine, swap(mine),
            scratch=scratches(levels, high // SUB, cols, high),
        )
        pieces = [pieces[0]] + [around(pieces[shift], shift) for shift in range(1, levels)]
        others = []
    return call(functools.partial(place_kernel, levels, strip), struct(1, rows, cols), *pieces, *others)


def solution(mesh):
    sizes = tuple(mesh.shape[axis] for axis in ("tm", "sx", "sy"))
    in_specs = (
        P("tm", "sx", "sy"),
        P("sx", "sy"),
        P("sx", "sy"),
        P("sx", "sy"),
        P("tm", "sx", "sy"),
        P("sx", "sy"),
    )
    out_specs = P("tm", "sx", "sy")

    def whole(*args):
        return body(sizes, *args)

    return jax.shard_map(whole, mesh=mesh, in_specs=in_specs, out_specs=out_specs, check_vma=False)
```
